32 devices in a mesh: groups: 2 (over y), seq: 4 (over z), sample: 2 (over x), vocab: 2 (over core).
Axes of the slice: x: 2, y: 2, z: 4, core: 2. Of those that a mesh axis runs over, the one named last changes fastest.
Arguments:
- queries: bfloat16 [16, 256, 1792], P(('groups', 'sample'), 'seq', 'vocab'), parts along dimension 0, may hold values from -130 to 130
- key_states: bfloat16 [16, 256, 256], P(('groups', 'sample'), 'seq', 'vocab'), parts along dimension 0, may hold values from -8 to 8
- value_states: bfloat16 [16, 256, 256], P(('groups', 'sample'), 'seq', 'vocab'), parts along dimension 0, may hold values from -6 to 6
- residual: bfloat16 [16, 256, 1792], P(('groups', 'sample'), 'seq'), parts along dimension 0, may hold values from -3 to 3
- out_weight: bfloat16 [1792, 1792], P('vocab'), may hold values from -0.5 to 0.5
- norm_gain: float32 [1792], replicated, may hold values from 0.5 to 1.5
- vocab_head: bfloat16 [81920, 1792], P(('seq', 'sample', 'vocab')), may hold values from -21 to 21
- targets: int32 [16, 256], P(('groups', 'sample')), parts along dimension 0, may hold values from 0 to 81919
- scored_slots: int32 [16, 64], P(('groups', 'sample')), parts along dimension 0, may hold values from -1 to 255, as said below
- lengths: int32 [16], P(('groups', 'sample')), parts along dimension 0, may hold values from 64 to 256
- rewards: int32 [16], P(('groups', 'sample')), parts along dimension 0, may hold values from 0 to 4
Outputs:
- token_logprobs: float32 [16, 64], P(('groups', 'sample'), 'seq'), parts along dimension 0
- seq_scores: float32 [16], P(('groups', 'sample')), parts along dimension 0
- advantages: float32 [16], P(('groups', 'sample')), parts along dimension 0
- objective: float32 [2], P('groups'), parts along dimension 0
The draws below stay inside these ranges and needn't reach their ends.
There are 2 independent parts, one for each index of `groups`. The reference program is written for one: setup_inputs(seed, part) draws one part's arguments, and reference() takes and returns one part's arrays. A program takes and returns all parts, laid end to end along the dimension named above; an argument that names none is the same for every part. Nothing has to cross between parts.
Inputs may be any that keep to these rules, and one draw needn't show every extreme that they name: `scored_slots`: slots b * 16 to (b + 1) * 16 - 1 of a completion hold distinct positions of b * 64 to (b + 1) * 64 - 1 in rising order, followed by -1 in unused slots; every completion fills all 16 slots of some block; positions not listed are not scored. Positions from lengths[i] on are padding.
All inputs are finite; a program needn't handle non-finite values.
Results may differ from the reference program's by a relative error of at most 0.0085.
Values may be sent and summed in bfloat16 or wider, within the bound.
No kernel may reach another device: no remote copies, remote signals or barrier semaphores. Data moves between devices by JAX's collectives and lax.ppermute only.
A program may use at most 128 MiB of HBM per device.

```python
import math
import jax
import jax.numpy as jnp
import numpy as np
from jax import lax

D = 1792
HQ = 14
HK = 2
HD = 128
V = 81920
K = 8
CH = 64
L = 256
CAP = 16


def attention_inputs(key):
    query_draw = jnp.clip(jax.random.normal(jax.random.fold_in(key, 11), (K, L, HQ * HD), jnp.float32), -6.0, 6.0)
    key_draw = jnp.clip(jax.random.normal(jax.random.fold_in(key, 12), (K, L, HK * HD), jnp.float32), -6.0, 6.0)
    return (query_draw, key_draw)


def draw_queries(key, part):
    return attention_inputs(key)[0].astype(jnp.bfloat16)


def draw_key_states(key, part):
    return attention_inputs(key)[1].astype(jnp.bfloat16)


def draw_vocab_head(key, part):
    base = jnp.clip(jax.random.normal(jax.random.fold_in(key, 21), (V, D), jnp.float32), -6.0, 6.0) * (3.0 / math.sqrt(D))
    return base.astype(jnp.bfloat16)


def draw_scored_slots(key, part):
    blocks = L // CH
    full_block = jax.random.randint(jax.random.fold_in(key, 31), (K,), 0, blocks)
    counts = jax.random.randint(jax.random.fold_in(key, 32), (K, blocks), CAP // 3, CAP + 1)
    counts = jnp.where(jnp.arange(blocks)[None, :] == full_block[:, None], CAP, counts)
    block_keys = jax.random.split(jax.random.fold_in(key, 33), K * blocks)
    picks = jax.vmap(lambda one_key: jnp.sort(jax.random.permutation(one_key, CH)[:CAP]))(block_keys)
    positions = picks.reshape(K, blocks, CAP) + (jnp.arange(blocks) * CH)[None, :, None]
    used = jnp.arange(CAP)[None, None, :] < counts[:, :, None]
    return jnp.where(used, positions, -1).reshape(K, blocks * CAP).astype(jnp.int32)


def with_ends(values, rng, least, largest):
    dims = values.shape
    spot = [jax.random.randint(jax.random.fold_in(rng, axis), (), 0, dims[axis]) for axis in range(len(dims))]
    values = values.at[tuple(spot)].set(least)
    longest = dims.index(max(dims))
    spot[longest] = (spot[longest] + 1) % dims[longest]
    return values.at[tuple(spot)].set(largest)


def shard_levels(own_key, extent, cuts, smallest, high):
    def one(axis_at, blocks):
        steps = jax.random.uniform(jax.random.fold_in(jax.random.fold_in(own_key, 6), axis_at), (blocks,), jnp.float32, smallest / len(cuts), high / len(cuts))
        return jnp.repeat(jnp.exp(steps), extent[axis_at] // blocks).reshape((-1,) + (1,) * (len(extent) - axis_at - 1))

    level = one(*cuts[0])
    for cut in cuts[1:]:
        level = level * one(*cut)
    return level


def skewed_wide(rng, extent, amount, slope):
    weights = [min(1 << octave, amount + 1 - (1 << octave)) * (1 << 20) // math.isqrt((1 << octave) ** slope) + 1 for octave in range((amount + 1).bit_length()) if 1 << octave <= amount]
    scale = 1 + sum(weights) // (1 << 30)
    table = np.cumsum(np.array([max(1, weight // scale) for weight in weights]))
    pick = jax.random.randint(jax.random.fold_in(rng, 1), extent, 0, int(table[len(weights) - 1]))
    start = jnp.left_shift(1, jnp.searchsorted(jnp.asarray(table, jnp.int32), pick, side="right").astype(jnp.int32))
    standing = start - 1 + jax.random.randint(jax.random.fold_in(rng, 4), extent, 0, 1 << 30) % jnp.minimum(start, amount + 1 - start)
    return jax.random.permutation(jax.random.fold_in(rng, 2), amount)[standing].astype(jnp.int32)


def scatter_about(own_key, shape, scale, reach, cuts=(), kind=jnp.bfloat16):
    gain = shard_levels(own_key, shape, cuts, -0.22, 0.18) if cuts else 1.0
    entries = jax.random.normal(own_key, shape, jnp.float32) * scale * gain
    return jnp.minimum(jnp.maximum(entries, -reach), reach).astype(kind)


def setup_inputs(seed: int = 0, part: int = 0) -> dict:
    key_list = jax.random.split(jax.random.key(seed), 12)
    own_keys = jax.random.split(jax.random.fold_in(key_list[11], part), 12)
    return {
        "queries": draw_queries(jax.random.fold_in(jax.random.fold_in(key_list[11], part), 71), part),
        "key_states": draw_key_states(jax.random.fold_in(jax.random.fold_in(key_list[11], part), 71), part),
        "value_states": scatter_about(own_keys[2], (K, L, HK * HD), 1.0, 6.0, ((0, 2), (1, 4), (2, 2))),
        "residual": scatter_about(own_keys[3], (K, L, D), 0.5, 3.0, ((0, 2), (1, 4))),
        "out_weight": scatter_about(key_list[4], (HQ * HD, D), (HQ * HD // 16) ** -0.5, 0.5, ((0, 2),)),
        "norm_gain": jnp.clip(1.0 + 0.1 * jax.random.normal(key_list[5], (D,), jnp.float32), 0.5, 1.5),
        "vocab_head": draw_vocab_head(jax.random.fold_in(key_list[11], 71), part),
        "targets": with_ends(skewed_wide(own_keys[7], (K, L), V, 2), jax.random.fold_in(own_keys[7], 3), 0, V - 1).astype(jnp.int32),
        "scored_slots": draw_scored_slots(jax.random.fold_in(jax.random.fold_in(key_list[11], part), 71), part),
        "lengths": with_ends(jax.random.randint(own_keys[9], (K,), L // 4, L + 1), jax.random.fold_in(own_keys[9], 1), L // 4, L).astype(jnp.int32),
        "rewards": with_ends(jax.random.randint(own_keys[10], (K,), 0, 5), jax.random.fold_in(own_keys[10], 1), 0, 4).astype(jnp.int32),
    }


def attend_sample(inputs):
    query_rows, key_rows, value_rows = inputs
    seq_len = query_rows.shape[0]
    group_size = HQ // HK
    query_view = query_rows.reshape(seq_len, HK, group_size, HD).astype(jnp.float32)
    key_view = key_rows.reshape(seq_len, HK, HD).astype(jnp.float32)
    value_view = value_rows.reshape(seq_len, HK, HD).astype(jnp.float32)
    scores = jnp.einsum('tkgd,skd->tkgs', query_view, key_view) * HD ** (-0.5)
    positions = jnp.arange(seq_len, dtype=jnp.int32)
    allowed = (positions[None, :] <= positions[:, None])[:, None, None, :]
    masked = jnp.where(allowed, scores, -1e+30)
    top_score = lax.optimization_barrier(jnp.max(masked, axis=-1, keepdims=True))
    exponent = jnp.where(allowed, jnp.exp(masked - top_score), 0.0)
    weight_sum = lax.optimization_barrier(jnp.sum(exponent, axis=-1))
    rounded = lax.optimization_barrier(exponent.astype(jnp.bfloat16))
    mixed = jnp.einsum('tkgs,skd->tkgd', rounded.astype(jnp.float32), value_view)
    return (mixed / weight_sum[..., None]).reshape(seq_len, HQ * HD).astype(jnp.bfloat16)

def score_rows(normed_rows, wanted, vocab_head):
    logits = jnp.dot(normed_rows, vocab_head.T, preferred_element_type=jnp.float32)
    top_score = lax.optimization_barrier(jnp.max(logits, axis=-1))
    weight_sum = lax.optimization_barrier(jnp.sum(jnp.exp(logits - top_score[:, None]), axis=-1))
    picked = jnp.take_along_axis(logits, wanted[:, None].astype(jnp.int32), axis=1)[:, 0]
    return picked - (top_score + jnp.log(weight_sum))

def reference(queries, key_states, value_states, residual, out_weight, norm_gain, vocab_head, targets, scored_slots, lengths, rewards):
    attended = lax.map(attend_sample, (queries, key_states, value_states))
    sample_count, seq_len, model_width = residual.shape
    partial_value = jnp.dot(attended.reshape(sample_count * seq_len, HQ * HD), out_weight, preferred_element_type=jnp.float32)
    hidden = residual.reshape(sample_count * seq_len, model_width).astype(jnp.float32) + partial_value
    power = lax.optimization_barrier(jnp.mean(hidden * hidden, axis=-1, keepdims=True))
    normed = (hidden * lax.rsqrt(power + 1e-06) * norm_gain).astype(jnp.bfloat16)
    normed = normed.reshape(sample_count, seq_len, model_width)
    slot_pos = jnp.maximum(scored_slots, 0).astype(jnp.int32)
    chosen = jnp.take_along_axis(normed, slot_pos[:, :, None], axis=1)
    wanted = jnp.take_along_axis(targets, slot_pos, axis=1)
    logprob = lax.map(lambda pair: score_rows(pair[0], pair[1], vocab_head), (chosen, wanted))
    scored = (scored_slots >= 0) & (scored_slots < lengths[:, None])
    token_logprobs = jnp.where(scored, logprob, 0.0)
    seq_scores = lax.optimization_barrier(jnp.sum(token_logprobs, axis=-1)) / seq_len
    reward_vals = rewards.astype(jnp.float32)
    reward_sum = jnp.sum(reward_vals)
    advantages = reward_vals - (reward_sum - reward_vals) / (K - 1)
    objective = -(jnp.sum(advantages * seq_scores) / K).reshape(1)
    return (token_logprobs, seq_scores, advantages, objective)
```

```python
import functools

import jax
import jax.numpy as jnp
from jax import lax
from jax.experimental import pallas as pl
from jax.experimental.pallas import tpu as pltpu
from jax.sharding import PartitionSpec as P

HD = 128
F32 = jnp.float32
BF16 = jnp.bfloat16
FLOOR = -1e30
CELL = ("seq", "sample", "vocab")


def vmem():
    return pl.BlockSpec(memory_space=pltpu.VMEM)


def smem():
    return pl.BlockSpec(memory_space=pltpu.SMEM)


def call(body, outs, ins, in_specs, out_specs=None, scratch=(), limit=24):
    return pl.pallas_call(
        body,
        out_shape=outs,
        in_specs=in_specs,
        out_specs=jax.tree.map(lambda _: vmem(), outs) if out_specs is None else out_specs,
        scratch_shapes=list(scratch),
        compiler_params=pltpu.CompilerParams(vmem_limit_bytes=limit * 2**20),
    )(*ins)


def iota(shape, dim):
    return lax.broadcasted_iota(jnp.int32, shape, dim)


def own_slot_column(slots_row, seq_at, cap):
    total = slots_row.shape[1]
    hit = iota((cap, total), 1) == iota((cap, total), 0) + seq_at * cap
    return jnp.sum(jnp.where(hit, slots_row, 0), axis=1, keepdims=True)


def prep_kernel(slots, targets, lengths, rewards, queries, residual, q_out, r_out, meta_out):
    samples, block, width = queries.shape
    total, length = slots.shape[1], targets.shape[1]
    heads = width // HD
    cap = r_out.shape[0] // samples
    seq_at = lax.axis_index("seq")
    lanes = meta_out.shape[1]
    reward_row = jnp.zeros((1, lanes), jnp.int32)
    wanted_rows = []
    for i in range(samples):
        row = slots[i : i + 1, :]
        local = jnp.clip(own_slot_column(row, seq_at, cap) - seq_at * block, 0, block - 1)
        onehot = (iota((cap, block), 1) == local).astype(F32).astype(BF16)
        picked = jnp.dot(onehot, queries[i], preferred_element_type=F32).astype(BF16)
        for h in range(heads):
            q_out[i, h * cap : (h + 1) * cap, :] = picked[:, h * HD : (h + 1) * HD]
        r_out[i * cap : (i + 1) * cap, :] = jnp.dot(
            onehot, residual[i], preferred_element_type=F32
        ).astype(BF16)
        eye = iota((total, total), 0) == iota((total, total), 1)
        column = jnp.sum(jnp.where(eye, jnp.maximum(row, 0), 0), axis=1, keepdims=True)
        spot = iota((total, length), 1) == column
        found = jnp.sum(jnp.where(spot, targets[i : i + 1, :], 0), axis=1, keepdims=True)
        wanted = jnp.sum(jnp.where(eye, found, 0), axis=0, keepdims=True)
        scored = (row >= 0) & (row < lengths[i])
        wanted_rows.append(jnp.where(scored, wanted, -1))
        reward_row = jnp.where(iota((1, lanes), 1) == i, rewards[i], reward_row)
    meta_out[0:1, :] = jnp.concatenate(wanted_rows, axis=1)
    meta_out[1:2, :] = reward_row


def attend_kernel(offsets, slots, queries, weight, *refs):
    blocks, out = refs[:-1], refs[-1]
    samples, stacked, _ = queries.shape
    block_len, kv_width = blocks[0].shape[1], blocks[0].shape[2]
    kv_heads = kv_width // (2 * HD)
    heads = weight.shape[0] // HD
    cap = stacked // heads
    group = heads // kv_heads
    span = block_len * len(blocks)
    seq_at = lax.axis_index("seq")
    lane = iota((1, span), 1)
    key_pos = lane
    if len(blocks) > 1:
        key_pos = jnp.zeros((1, span), jnp.int32)
        for n, flip in enumerate(offsets):
            start = jnp.bitwise_xor(seq_at, flip) * block_len
            key_pos = jnp.where(lane // block_len == n, lane - n * block_len + start, key_pos)
    rows = []
    for i in range(samples):
        column = jnp.maximum(own_slot_column(slots[i : i + 1, :], seq_at, cap), 0)
        reach = jnp.concatenate([column] * group, axis=0)
        allowed = key_pos <= reach
        pieces = []
        for g in range(kv_heads):
            left, right = g * HD, kv_width // 2 + g * HD
            keys = jnp.concatenate([b[i, :, left : left + HD] for b in blocks], axis=0)
            values = jnp.concatenate([b[i, :, right : right + HD] for b in blocks], axis=0)
            query = queries[i, g * group * cap : (g + 1) * group * cap, :]
            scores = lax.dot_general(
                query, keys, (((1,), (1,)), ((), ())), preferred_element_type=F32
            ) * HD ** (-0.5)
            scores = jnp.where(allowed, scores, FLOOR)
            top = jnp.max(scores, axis=1, keepdims=True)
            weights = jnp.where(allowed, jnp.exp(scores - top), 0.0)
            total = jnp.sum(weights, axis=1, keepdims=True)
            mixed = jnp.dot(weights.astype(BF16), values, preferred_element_type=F32)
            mixed = (mixed / total).astype(BF16)
            pieces += [mixed[h * cap : (h + 1) * cap, :] for h in range(group)]
        rows.append(jnp.concatenate(pieces, axis=1))
    attended = jnp.concatenate(rows, axis=0)
    out[...] = jnp.dot(attended, weight[...], preferred_element_type=F32).astype(BF16)


def norm_kernel(mine, other, residual, gain, full, half):
    hidden = residual[...].astype(F32) + (mine[...].astype(F32) + other[...].astype(F32))
    power = jnp.mean(hidden * hidden, axis=-1, keepdims=True)
    full[...] = (hidden * lax.rsqrt(power + 1e-06) * gain[...]).astype(BF16)
    if half is not None:
        count = half.shape[0]
        start = pl.multiple_of(lax.axis_index("vocab") * count, count)
        half[...] = full[pl.ds(start, count), :]


def fold(logits, wanted, first_row, top_ref, sum_ref, pick_ref):
    count, width = logits.shape
    tiles = logits.reshape(count // 8, 8, width)
    old = top_ref[...]
    new = jnp.maximum(old, jnp.max(tiles, axis=0))
    grown = jnp.sum(jnp.exp(tiles - new[None]), axis=0)
    sum_ref[...] = sum_ref[...] * jnp.exp(old - new) + grown
    top_ref[...] = new
    rows = iota(tiles.shape, 0) * 8 + iota(tiles.shape, 1)
    hit = rows == (wanted - first_row)[None]
    pick_ref[...] += jnp.sum(jnp.where(hit, tiles, 0.0), axis=0)


def score_tile(head, states, wanted, buffers, top_ref, sum_ref, pick_ref, step, unroll, base):
    top_ref[...] = jnp.full(top_ref.shape, FLOOR, F32)
    sum_ref[...] = jnp.zeros(sum_ref.shape, F32)
    pick_ref[...] = jnp.zeros(pick_ref.shape, F32)
    buffers[1][...] = jnp.full(buffers[1].shape, FLOOR, F32)
    local = wanted - base
    local = jnp.where((local >= 0) & (local < head.shape[0]), local, -(1 << 30))
    local = jnp.broadcast_to(local, top_ref.shape)

    def body(at, carry):
        for j in range(unroll):
            first = at * (unroll * step) + j * step
            block = head[pl.ds(pl.multiple_of(first, step), step), :]
            logits = lax.dot_general(
                block, states[...], (((1,), (1,)), ((), ())), preferred_element_type=F32
            )
            fold(buffers[(j + 1) % 2][...], local, first - step, top_ref, sum_ref, pick_ref)
            buffers[j % 2][...] = logits
        return carry

    total = head.shape[0]
    lax.fori_loop(0, total // (unroll * step), body, 0)
    fold(buffers[(unroll - 1) % 2][...], local, total - step, top_ref, sum_ref, pick_ref)
    top = jnp.max(top_ref[...], axis=0, keepdims=True)
    scale = jnp.exp(top_ref[...] - top)
    total = jnp.sum(sum_ref[...] * scale, axis=0, keepdims=True)
    return top, total, jnp.sum(pick_ref[...], axis=0, keepdims=True)


def vocab_base(shard_rows):
    owner = lax.axis_index("seq") * lax.axis_size("sample") + lax.axis_index("sample")
    return (owner * lax.axis_size("vocab") + lax.axis_index("vocab")) * shard_rows


def steps_of(shard_rows):
    for step in (256, 128, 64, 32, 16, 8):
        if shard_rows % (2 * step) == 0:
            unroll = 10 if shard_rows % (10 * step) == 0 else 2
            return step, unroll
    raise ValueError("head rows")


def column_kernel(places, samples, step, unroll, last, head, meta, *refs):
    before, refs = (refs[0], refs[1:]) if last else (None, refs)
    blocks, out = refs[: len(places)], refs[len(places)]
    states, buf_a, buf_b, top_ref, sum_ref, pick_ref = refs[len(places) + 1 :]
    slot_total = states.shape[0] // samples
    seq_at, core = lax.axis_index("seq"), lax.axis_index("vocab")
    for ref, (kind, part) in zip(blocks, places):
        if kind == "split":
            mine, other = (1, 3) if part == 0 else (3, 1)
            owner = jnp.bitwise_xor(seq_at, jnp.where(core == 0, mine, other))
        else:
            owner = jnp.bitwise_xor(seq_at, kind)
        held = samples
        first = 0
        if kind != "split" and part is not None:
            held = samples // 2
            first = jnp.bitwise_xor(core, part) * held
        cap = ref.shape[0] // held
        for i in range(held):
            start = pl.multiple_of((first + i) * slot_total + owner * cap, cap)
            states[pl.ds(start, cap), :] = ref[i * cap : (i + 1) * cap, :]
    parts = score_tile(
        head, states, meta[0:1, :], (buf_a, buf_b), top_ref, sum_ref, pick_ref,
        step, unroll, vocab_base(head.shape[0]),
    )
    rows = jnp.concatenate([*parts, parts[0]], axis=0)
    if not last:
        out[...] = rows
    else:
        swapped = lax.axis_index("sample") == 1
        low = jnp.where(swapped, rows, before[...])
        high = jnp.where(swapped, before[...], rows)
        both = jnp.concatenate([low, high], axis=0)
        out[...] = jnp.broadcast_to(both[None], out.shape)


def column_scores(head, meta, blocks, places, samples, before=None):
    step, unroll = steps_of(head.shape[0])
    rows = meta.shape[1]
    last = before is not None
    peers = 1
    for axis in CELL:
        peers *= lax.axis_size(axis)
    out = jax.ShapeDtypeStruct((peers, 8, rows) if last else (4, rows), F32)
    extra = [before] if last else []
    return call(
        functools.partial(column_kernel, places, samples, step, unroll, last),
        out,
        [head, meta, *extra, *blocks],
        [vmem()] * (2 + len(extra) + len(blocks)),
        scratch=[pltpu.VMEM((rows, head.shape[1]), BF16)]
        + [pltpu.VMEM((step, rows), F32)] * 2
        + [pltpu.VMEM((8, rows), F32)] * 3,
        limit=36,
    )


def tile_kernel(step, unroll, head, states, wanted, out, buf_a, buf_b, top_ref, sum_ref, pick_ref):
    parts = score_tile(
        head, states, wanted[...], (buf_a, buf_b), top_ref, sum_ref, pick_ref,
        step, unroll, vocab_base(head.shape[0]),
    )
    out[...] = jnp.concatenate([*parts, parts[0]], axis=0)


def tiled_scores(head, states, wanted):
    step, unroll = steps_of(head.shape[0])
    count, width = states.shape
    tile = next(n for n in (256, 128, count) if count % n == 0)
    return pl.pallas_call(
        functools.partial(tile_kernel, step, unroll),
        grid=(count // tile,),
        out_shape=jax.ShapeDtypeStruct((4, count), F32),
        in_specs=[
            pl.BlockSpec(head.shape, lambda i: (0, 0)),
            pl.BlockSpec((tile, width), lambda i: (i, 0)),
            pl.BlockSpec((1, tile), lambda i: (0, i)),
        ],
        out_specs=pl.BlockSpec((4, tile), lambda i: (0, i)),
        scratch_shapes=[pltpu.VMEM((step, tile), F32)] * 2 + [pltpu.VMEM((8, tile), F32)] * 3,
        compiler_params=pltpu.CompilerParams(
            dimension_semantics=("arbitrary",), vmem_limit_bytes=52 * 2**20
        ),
    )(head, states, wanted)


def close_kernel(relative, prompts, length, stats, rewards, *refs):
    metas, (tokens_out, scores_out, advantages_out, objective_out) = refs[:-4], refs[-4:]
    metas = [ref[...] for ref in metas]
    samples, cap = tokens_out.shape
    lanes = metas[0].shape[1]
    slot_total = lanes // samples
    columns = len(metas)
    where = lax.axis_index("sample")
    if relative:
        metas = [jnp.where(where == k, metas[0], metas[1]) for k in range(columns)]
    tokens = []
    for k in range(columns):

        def gathered(row):
            return jnp.concatenate([stats[s, row : row + 1, :] for s in range(stats.shape[0])], axis=0)

        tops = gathered(4 * k)
        top = jnp.max(tops, axis=0, keepdims=True)
        total = jnp.sum(gathered(4 * k + 1) * jnp.exp(tops - top), axis=0, keepdims=True)
        pick = jnp.sum(gathered(4 * k + 2), axis=0, keepdims=True)
        tokens.append(jnp.where(metas[k][0:1, :] >= 0, pick - (top + jnp.log(total)), 0.0))
    paid = [meta[1:2, :].astype(F32) for meta in metas]
    reward_sum = functools.reduce(lambda a, b: a + b, [jnp.sum(row) for row in paid])
    lane = iota((1, lanes), 1)
    objective = jnp.float32(0)
    for k in range(columns):
        for i in range(samples):
            score = jnp.sum(tokens[k][:, i * slot_total : (i + 1) * slot_total]) / length
            reward = jnp.sum(jnp.where(lane == i, paid[k], 0.0))
            objective += (reward - (reward_sum - reward) / (prompts - 1)) * score

            @pl.when(where == k)
            def _(score=score, i=i):
                scores_out[i] = score

    for i in range(samples):
        mine = rewards[i].astype(F32)
        advantages_out[i] = mine - (reward_sum - mine) / (prompts - 1)
    objective_out[0] = -(objective / prompts)
    mine = tokens[0]
    for k in range(1, columns):
        mine = jnp.where(where == k, tokens[k], mine)
    seq_at = lax.axis_index("seq")
    for i in range(samples):
        row = mine[:, i * slot_total : (i + 1) * slot_total]
        piece = row[:, :cap]
        for n in range(1, slot_total // cap):
            piece = jnp.where(seq_at == n, row[:, n * cap : (n + 1) * cap], piece)
        tokens_out[i : i + 1, :] = piece


def close(stats, rewards, metas, relative, samples, cap, length):
    prompts = samples * lax.axis_size("sample")
    outs = (
        jax.ShapeDtypeStruct((samples, cap), F32),
        jax.ShapeDtypeStruct((samples,), F32),
        jax.ShapeDtypeStruct((samples,), F32),
        jax.ShapeDtypeStruct((1,), F32),
    )
    return call(
        functools.partial(close_kernel, relative, prompts, length),
        outs,
        [stats, rewards, *metas],
        [vmem(), smem()] + [vmem()] * len(metas),
        out_specs=(vmem(), smem(), smem(), smem()),
    )


def shards(
    queries, key_states, value_states, residual, out_weight, norm_gain,
    vocab_head, targets, scored_slots, lengths, rewards,
):
    samples, block, width = queries.shape
    model_width = out_weight.shape[1]
    seq_size, sample_size, vocab_size = (lax.axis_size(axis) for axis in CELL)
    cap = scored_slots.shape[1] // seq_size
    length = targets.shape[1]
    rows = samples * cap
    lanes = samples * scored_slots.shape[1]
    short = (seq_size, sample_size, vocab_size) == (4, 2, 2) and samples % 2 == 0

    def send(array, target):
        pairs = []
        for z in range(seq_size):
            for x in range(sample_size):
                for c in range(vocab_size):
                    to_z, to_x, to_c = target(z, x, c)
                    source = (z * sample_size + x) * vocab_size + c
                    pairs.append((source, (to_z * sample_size + to_x) * vocab_size + to_c))
        return lax.ppermute(array, CELL, pairs)

    def across(array):
        return send(array, lambda z, x, c: (z, x, c ^ 1))

    def beside(array):
        return send(array, lambda z, x, c: (z, x ^ 1, c))

    pair = jnp.concatenate([key_states, value_states], axis=-1)
    if short:
        offsets = (0, 1, 3, 2)
        far = send(pair, lambda z, x, c: (z ^ 2, x, c))
        near = send(pair, lambda z, x, c: (z ^ 1, x, c))
        wrap = send(pair, lambda z, x, c: (z ^ 3, x, c))
        blocks = [pair, near, wrap, far]
    else:
        offsets = (0,)
        blocks = [lax.all_gather(pair, "seq", axis=1, tiled=True)]
    heads = width // HD
    picked, picked_resid, meta = call(
        prep_kernel,
        (
            jax.ShapeDtypeStruct((samples, heads * cap, HD), BF16),
            jax.ShapeDtypeStruct((rows, model_width), BF16),
            jax.ShapeDtypeStruct((2, lanes), jnp.int32),
        ),
        [scored_slots, targets, lengths, rewards, queries, residual],
        [vmem(), vmem(), smem(), smem(), vmem(), vmem()],
    )
    partial_value = call(
        functools.partial(attend_kernel, offsets),
        jax.ShapeDtypeStruct((rows, model_width), BF16),
        [scored_slots, picked, out_weight, *blocks],
        [vmem()] * (3 + len(blocks)),
    )
    gain = norm_gain.reshape(1, model_width)
    if short:
        other_meta = beside(meta)
        normed, half = call(
            norm_kernel,
            (
                jax.ShapeDtypeStruct((rows, model_width), BF16),
                jax.ShapeDtypeStruct((rows // 2, model_width), BF16),
            ),
            [partial_value, across(partial_value), picked_resid, gain],
            [vmem()] * 4,
        )
        far = send(half, lambda z, x, c: (z ^ 2, x, c))
        split = send(normed, lambda z, x, c: (z ^ (1, 3)[c], x, c))
        side = beside(half)
        split_side = beside(split)
        far_side = beside(far)
        first = column_scores(
            vocab_head, meta,
            [normed, split, across(split), far, across(far)],
            [(0, None), ("split", 0), ("split", 1), (2, 0), (2, 1)],
            samples,
        )
        stats = column_scores(
            vocab_head, other_meta,
            [side, across(side), split_side, across(split_side), far_side, across(far_side)],
            [(0, 0), (0, 1), ("split", 0), ("split", 1), (2, 0), (2, 1)],
            samples,
            before=first,
        )
        stats = lax.all_to_all(stats, CELL, 0, 0, tiled=True)

        return close(stats, rewards, [meta, other_meta], True, samples, cap, length)
    summed = lax.psum(partial_value, "vocab")
    normed = call(
        lambda a, b, r, g, out: norm_kernel(a, b, r, g, out, None),
        jax.ShapeDtypeStruct((rows, model_width), BF16),
        [summed, jnp.zeros_like(summed), picked_resid, gain],
        [vmem()] * 4,
    )
    every = lax.all_gather(normed.reshape(samples, cap, model_width), "seq", axis=1, tiled=True)
    every = lax.all_gather(every, "sample", axis=0, tiled=True).reshape(-1, model_width)
    metas = lax.all_gather(meta, "sample", axis=0)
    stats = tiled_scores(vocab_head, every, metas[:, 0, :].reshape(1, -1))
    top = lax.pmax(stats[0], CELL)
    total, pick = lax.psum((stats[1] * jnp.exp(stats[0] - top), stats[2]), CELL)
    stats = jnp.stack([top, total, pick, top]).reshape(4, sample_size, lanes)
    stats = stats.transpose(1, 0, 2).reshape(1, sample_size * 4, lanes)
    metas = [metas[k] for k in range(sample_size)]
    return close(stats, rewards, metas, False, samples, cap, length)


def solution(mesh):
    in_specs = (
        P(("groups", "sample"), "seq", "vocab"),
        P(("groups", "sample"), "seq", "vocab"),
        P(("groups", "sample"), "seq", "vocab"),
        P(("groups", "sample"), "seq", None),
        P("vocab", None),
        P(),
        P(("seq", "sample", "vocab"), None),
        P(("groups", "sample"), None),
        P(("groups", "sample"), None),
        P(("groups", "sample")),
        P(("groups", "sample")),
    )
    out_specs = (
        P(("groups", "sample"), "seq"),
        P(("groups", "sample")),
        P(("groups", "sample")),
        P("groups"),
    )
    return jax.shard_map(shards, mesh=mesh, in_specs=in_specs, out_specs=out_specs, check_vma=False)
```

```python
import functools

import jax
import jax.numpy as jnp
from jax import lax
from jax.experimental import pallas as pl
from jax.experimental.pallas import tpu as pltpu
from jax.sharding import PartitionSpec as P

HD = 128
F32 = jnp.float32
BF16 = jnp.bfloat16
FLOOR = -1e30
CELL = ("seq", "sample", "vocab")


def vmem():
    return pl.BlockSpec(memory_space=pltpu.VMEM)


def hbm():
    return pl.BlockSpec(memory_space=pltpu.HBM)


def keep(array):
    return pltpu.with_memory_space_constraint(array, pltpu.HBM)


def smem():
    return pl.BlockSpec(memory_space=pltpu.SMEM)


def call(body, outs, ins, in_specs, out_specs=None, scratch=(), limit=12, flops=None):
    cost = None
    if flops is not None:
        cost = pl.CostEstimate(flops=flops, bytes_accessed=0, transcendentals=0)
    return pl.pallas_call(
        body,
        cost_estimate=cost,
        out_shape=outs,
        in_specs=in_specs,
        out_specs=jax.tree.map(lambda _: vmem(), outs) if out_specs is None else out_specs,
        scratch_shapes=list(scratch),
        compiler_params=pltpu.CompilerParams(vmem_limit_bytes=limit * 2**20),
    )(*ins)


def iota(shape, dim):
    return lax.broadcasted_iota(jnp.int32, shape, dim)


def own_slot_column(slots_row, seq_at, cap):
    total = slots_row.shape[1]
    hit = iota((cap, total), 1) == iota((cap, total), 0) + seq_at * cap
    return jnp.sum(jnp.where(hit, slots_row, 0), axis=1, keepdims=True)


def pack_kernel(keys, values, out, sems):
    width = keys.shape[2]
    copies = [
        pltpu.make_async_copy(ref, out.at[:, :, pl.ds(n * width, width)], sems.at[n])
        for n, ref in enumerate((keys, values))
    ]
    for copy in copies:
        copy.start()
    for copy in copies:
        copy.wait()


def prep_kernel(
    count, slots_in, targets_in, lengths_in, rewards_in, queries, residual, weight, gain, head,
    slots, q_out, r_out, meta_out, weight_out, gain_out, head_out,
    targets, lengths, rewards, q_in, r_in, sems,
):
    samples, block, width = queries.shape
    total, length = slots.shape[1], targets.shape[1]
    heads = width // HD
    cap = r_out.shape[0] // samples
    seq_at = lax.axis_index("seq")
    lanes = meta_out.shape[1]
    step = head.shape[0] // count
    moves = [
        (slots_in, slots), (targets_in, targets), (lengths_in, lengths), (rewards_in, rewards),
        (queries, q_in), (residual, r_in), (weight, weight_out), (gain, gain_out),
    ]
    for n in range(count):
        moves.append((head.at[pl.ds(n * step, step), :], head_out.at[pl.ds(n * step, step), :]))
    copies = [pltpu.make_async_copy(a, b, sems.at[n]) for n, (a, b) in enumerate(moves)]
    for copy in copies:
        copy.start()
    for copy in copies[:4]:
        copy.wait()
    reward_row = jnp.zeros((1, lanes), jnp.int32)
    wanted_rows, onehots = [], []
    for i in range(samples):
        row = slots[i : i + 1, :]
        local = jnp.clip(own_slot_column(row, seq_at, cap) - seq_at * block, 0, block - 1)
        onehots.append((iota((cap, block), 1) == local).astype(F32).astype(BF16))
        eye = iota((total, total), 0) == iota((total, total), 1)
        column = jnp.sum(jnp.where(eye, jnp.maximum(row, 0), 0), axis=1, keepdims=True)
        spot = iota((total, length), 1) == column
        found = jnp.sum(jnp.where(spot, targets[i : i + 1, :], 0), axis=1, keepdims=True)
        wanted = jnp.sum(jnp.where(eye, found, 0), axis=0, keepdims=True)
        scored = (row >= 0) & (row < lengths[i])
        wanted_rows.append(jnp.where(scored, wanted, -1))
        reward_row = jnp.where(iota((1, lanes), 1) == i, rewards[i], reward_row)
    meta_out[0:1, :] = jnp.concatenate(wanted_rows, axis=1)
    meta_out[1:2, :] = reward_row
    copies[4].wait()
    for i in range(samples):
        picked = jnp.dot(onehots[i], q_in[i], preferred_element_type=F32).astype(BF16)
        for h in range(heads):
            q_out[i, h * cap : (h + 1) * cap, :] = picked[:, h * HD : (h + 1) * HD]
    copies[5].wait()
    for i in range(samples):
        r_out[i * cap : (i + 1) * cap, :] = jnp.dot(
            onehots[i], r_in[i], preferred_element_type=F32
        ).astype(BF16)
    for copy in copies[6:]:
        copy.wait()


def attend_kernel(offsets, slots, queries, weight, *refs):
    blocks, out = refs[:-1], refs[-1]
    samples, stacked, _ = queries.shape
    block_len, kv_width = blocks[0].shape[1], blocks[0].shape[2]
    kv_heads = kv_width // (2 * HD)
    heads = weight.shape[0] // HD
    cap = stacked // heads
    group = heads // kv_heads
    span = block_len * len(blocks)
    seq_at = lax.axis_index("seq")
    lane = iota((1, span), 1)
    key_pos = lane
    if len(blocks) > 1:
        key_pos = jnp.zeros((1, span), jnp.int32)
        for n, flip in enumerate(offsets):
            start = jnp.bitwise_xor(seq_at, flip) * block_len
            key_pos = jnp.where(lane // block_len == n, lane - n * block_len + start, key_pos)
    rows = []
    for i in range(samples):
        column = jnp.maximum(own_slot_column(slots[i : i + 1, :], seq_at, cap), 0)
        reach = jnp.concatenate([column] * group, axis=0)
        allowed = key_pos <= reach
        pieces = []
        for g in range(kv_heads):
            left, right = g * HD, kv_width // 2 + g * HD
            keys = jnp.concatenate([b[i, :, left : left + HD] for b in blocks], axis=0)
            values = jnp.concatenate([b[i, :, right : right + HD] for b in blocks], axis=0)
            query = queries[i, g * group * cap : (g + 1) * group * cap, :]
            scores = lax.dot_general(
                query, keys, (((1,), (1,)), ((), ())), preferred_element_type=F32
            ) * HD ** (-0.5)
            scores = jnp.where(allowed, scores, FLOOR)
            top = jnp.max(scores, axis=1, keepdims=True)
            weights = jnp.where(allowed, jnp.exp(scores - top), 0.0)
            total = jnp.sum(weights, axis=1, keepdims=True)
            mixed = jnp.dot(weights.astype(BF16), values, preferred_element_type=F32)
            mixed = (mixed / total).astype(BF16)
            pieces += [mixed[h * cap : (h + 1) * cap, :] for h in range(group)]
        rows.append(jnp.concatenate(pieces, axis=1))
    attended = jnp.concatenate(rows, axis=0)
    out[...] = jnp.dot(attended, weight[...], preferred_element_type=F32).astype(BF16)


def norm_kernel(mine, other, residual, gain, full, half):
    hidden = residual[...].astype(F32) + (mine[...].astype(F32) + other[...].astype(F32))
    power = jnp.mean(hidden * hidden, axis=-1, keepdims=True)
    full[...] = (hidden * lax.rsqrt(power + 1e-06) * gain[...]).astype(BF16)
    if half is not None:
        count = half.shape[0]
        start = pl.multiple_of(lax.axis_index("vocab") * count, count)
        half[...] = full[pl.ds(start, count), :]


def fold(logits, wanted, first_row, top_ref, sum_ref, pick_ref):
    count, width = logits.shape
    tiles = logits.reshape(count // 8, 8, width)
    old = top_ref[...]
    new = jnp.maximum(old, jnp.max(tiles, axis=0))
    grown = jnp.sum(jnp.exp(tiles - new[None]), axis=0)
    sum_ref[...] = sum_ref[...] * jnp.exp(old - new) + grown
    top_ref[...] = new
    rows = iota(tiles.shape, 0) * 8 + iota(tiles.shape, 1)
    hit = rows == (wanted - first_row)[None]
    pick_ref[...] += jnp.sum(jnp.where(hit, tiles, 0.0), axis=0)


def score_tile(head, states, wanted, buffers, top_ref, sum_ref, pick_ref, step, unroll, base):
    top_ref[...] = jnp.full(top_ref.shape, FLOOR, F32)
    sum_ref[...] = jnp.zeros(sum_ref.shape, F32)
    pick_ref[...] = jnp.zeros(pick_ref.shape, F32)
    buffers[1][...] = jnp.full(buffers[1].shape, FLOOR, F32)
    local = wanted - base
    local = jnp.where((local >= 0) & (local < head.shape[0]), local, -(1 << 30))
    local = jnp.broadcast_to(local, top_ref.shape)

    def body(at, carry):
        for j in range(unroll):
            first = at * (unroll * step) + j * step
            block = head[pl.ds(pl.multiple_of(first, step), step), :]
            logits = lax.dot_general(
                block, states[...], (((1,), (1,)), ((), ())), preferred_element_type=F32
            )
            fold(buffers[(j + 1) % 2][...], local, first - step, top_ref, sum_ref, pick_ref)
            buffers[j % 2][...] = logits
        return carry

    total = head.shape[0]
    lax.fori_loop(0, total // (unroll * step), body, 0)
    fold(buffers[(unroll - 1) % 2][...], local, total - step, top_ref, sum_ref, pick_ref)
    top = jnp.max(top_ref[...], axis=0, keepdims=True)
    scale = jnp.exp(top_ref[...] - top)
    total = jnp.sum(sum_ref[...] * scale, axis=0, keepdims=True)
    return top + jnp.log(total), jnp.sum(pick_ref[...], axis=0, keepdims=True)


def vocab_base(shard_rows):
    owner = lax.axis_index("seq") * lax.axis_size("sample") + lax.axis_index("sample")
    return (owner * lax.axis_size("vocab") + lax.axis_index("vocab")) * shard_rows


def steps_of(shard_rows):
    for step in (256, 128, 64, 32, 16, 8):
        if shard_rows % (2 * step) == 0:
            unroll = 10 if shard_rows % (10 * step) == 0 else 2
            return step, unroll
    raise ValueError("head rows")


def column_kernel(places, samples, step, unroll, last, head, meta, *refs):
    before, refs = (refs[0], refs[1:]) if last else (None, refs)
    blocks, out = refs[: len(places)], refs[len(places)]
    states, buf_a, buf_b, top_ref, sum_ref, pick_ref = refs[len(places) + 1 :]
    slot_total = states.shape[0] // samples
    seq_at, core = lax.axis_index("seq"), lax.axis_index("vocab")
    for ref, (kind, part) in zip(blocks, places):
        if kind == "split":
            mine, other = (1, 3) if part == 0 else (3, 1)
            owner = jnp.bitwise_xor(seq_at, jnp.where(core == 0, mine, other))
        else:
            owner = jnp.bitwise_xor(seq_at, kind)
        held = samples
        first = 0
        if kind != "split" and part is not None:
            held = samples // 2
            first = jnp.bitwise_xor(core, part) * held
        cap = ref.shape[0] // held
        for i in range(held):
            start = pl.multiple_of((first + i) * slot_total + owner * cap, cap)
            states[pl.ds(start, cap), :] = ref[i * cap : (i + 1) * cap, :]
    parts = score_tile(
        head, states, meta[0:1, :], (buf_a, buf_b), top_ref, sum_ref, pick_ref,
        step, unroll, vocab_base(head.shape[0]),
    )
    rows = jnp.concatenate(parts, axis=0)
    if not last:
        out[...] = rows
    else:
        swapped = lax.axis_index("sample") == 1
        low = jnp.where(swapped, rows, before[...])
        high = jnp.where(swapped, before[...], rows)
        both = jnp.concatenate([low, high], axis=0)
        out[...] = jnp.broadcast_to(both[None], out.shape)


def column_scores(head, meta, blocks, places, samples, before=None):
    step, unroll = steps_of(head.shape[0])
    rows = meta.shape[1]
    last = before is not None
    peers = 1
    for axis in CELL:
        peers *= lax.axis_size(axis)
    out = jax.ShapeDtypeStruct((peers, 4, rows) if last else (2, rows), F32)
    extra = [before] if last else []
    return call(
        functools.partial(column_kernel, places, samples, step, unroll, last),
        out,
        [head, meta, *extra, *blocks],
        [vmem()] * (2 + len(extra) + len(blocks)),
        scratch=[pltpu.VMEM((rows, head.shape[1]), BF16)]
        + [pltpu.VMEM((step, rows), F32)] * 2
        + [pltpu.VMEM((8, rows), F32)] * 3,
        limit=12,
        flops=2 * rows * head.shape[0] * head.shape[1],
    )


def tile_kernel(step, unroll, head, states, wanted, out, buf_a, buf_b, top_ref, sum_ref, pick_ref):
    parts = score_tile(
        head, states, wanted[...], (buf_a, buf_b), top_ref, sum_ref, pick_ref,
        step, unroll, vocab_base(head.shape[0]),
    )
    out[...] = jnp.concatenate(parts, axis=0)


def tiled_scores(head, states, wanted):
    step, unroll = steps_of(head.shape[0])
    count, width = states.shape
    tile = next(n for n in (256, 128, count) if count % n == 0)
    return pl.pallas_call(
        functools.partial(tile_kernel, step, unroll),
        grid=(count // tile,),
        out_shape=jax.ShapeDtypeStruct((2, count), F32),
        in_specs=[
            pl.BlockSpec(head.shape, lambda i: (0, 0)),
            pl.BlockSpec((tile, width), lambda i: (i, 0)),
            pl.BlockSpec((1, tile), lambda i: (0, i)),
        ],
        out_specs=pl.BlockSpec((2, tile), lambda i: (0, i)),
        scratch_shapes=[pltpu.VMEM((step, tile), F32)] * 2 + [pltpu.VMEM((8, tile), F32)] * 3,
        compiler_params=pltpu.CompilerParams(
            dimension_semantics=("arbitrary",), vmem_limit_bytes=52 * 2**20
        ),
    )(head, states, wanted)


def close_kernel(relative, prompts, length, stats, *refs):
    metas, (tokens_out, scores_out, advantages_out, objective_out) = refs[:-4], refs[-4:]
    metas = [ref[...] for ref in metas]
    samples, cap = tokens_out.shape
    lanes = metas[0].shape[1]
    slot_total = lanes // samples
    columns = len(metas)
    where = lax.axis_index("sample")
    if relative:
        metas = [jnp.where(where == k, metas[0], metas[1]) for k in range(columns)]
    tokens = []
    for k in range(columns):

        def gathered(row):
            return jnp.concatenate([stats[s, row : row + 1, :] for s in range(stats.shape[0])], axis=0)

        logs = gathered(2 * k)
        top = jnp.max(logs, axis=0, keepdims=True)
        total = jnp.sum(jnp.exp(logs - top), axis=0, keepdims=True)
        pick = jnp.sum(gathered(2 * k + 1), axis=0, keepdims=True)
        tokens.append(jnp.where(metas[k][0:1, :] >= 0, pick - (top + jnp.log(total)), 0.0))
    paid = [meta[1:2, :].astype(F32) for meta in metas]
    reward_sum = functools.reduce(lambda a, b: a + b, [jnp.sum(row) for row in paid])
    lane = iota((1, lanes), 1)
    objective = jnp.float32(0)
    for k in range(columns):
        for i in range(samples):
            score = jnp.sum(tokens[k][:, i * slot_total : (i + 1) * slot_total]) / length
            reward = jnp.sum(jnp.where(lane == i, paid[k], 0.0))
            advantage = reward - (reward_sum - reward) / (prompts - 1)
            objective += advantage * score

            @pl.when(where == k)
            def _(score=score, advantage=advantage, i=i):
                scores_out[i] = score
                advantages_out[i] = advantage

    objective_out[0] = -(objective / prompts)
    mine = tokens[0]
    for k in range(1, columns):
        mine = jnp.where(where == k, tokens[k], mine)
    seq_at = lax.axis_index("seq")
    for i in range(samples):
        row = mine[:, i * slot_total : (i + 1) * slot_total]
        piece = row[:, :cap]
        for n in range(1, slot_total // cap):
            piece = jnp.where(seq_at == n, row[:, n * cap : (n + 1) * cap], piece)
        tokens_out[i : i + 1, :] = piece


def close(stats, metas, relative, samples, cap, length):
    prompts = samples * lax.axis_size("sample")
    outs = (
        jax.ShapeDtypeStruct((samples, cap), F32),
        jax.ShapeDtypeStruct((samples,), F32),
        jax.ShapeDtypeStruct((samples,), F32),
        jax.ShapeDtypeStruct((1,), F32),
    )
    return call(
        functools.partial(close_kernel, relative, prompts, length),
        outs,
        [stats, *metas],
        [vmem()] * (1 + len(metas)),
        out_specs=(vmem(), smem(), smem(), smem()),
    )


def shards(
    queries, key_states, value_states, residual, out_weight, norm_gain,
    vocab_head, targets, scored_slots, lengths, rewards,
):
    samples, block, width = queries.shape
    model_width = out_weight.shape[1]
    seq_size, sample_size, vocab_size = (lax.axis_size(axis) for axis in CELL)
    cap = scored_slots.shape[1] // seq_size
    length = targets.shape[1]
    rows = samples * cap
    lanes = samples * scored_slots.shape[1]
    short = (seq_size, sample_size, vocab_size) == (4, 2, 2) and samples % 2 == 0

    def send(array, target):
        pairs = []
        for z in range(seq_size):
            for x in range(sample_size):
                for c in range(vocab_size):
                    to_z, to_x, to_c = target(z, x, c)
                    source = (z * sample_size + x) * vocab_size + c
                    pairs.append((source, (to_z * sample_size + to_x) * vocab_size + to_c))
        return lax.ppermute(array, CELL, pairs)

    def across(array):
        return send(array, lambda z, x, c: (z, x, c ^ 1))

    def beside(array):
        return send(array, lambda z, x, c: (z, x ^ 1, c))

    kv_shape = (samples, block, 2 * key_states.shape[2])
    pair = call(
        pack_kernel,
        jax.ShapeDtypeStruct(kv_shape, BF16),
        [keep(key_states), keep(value_states)],
        [hbm(), hbm()],
        scratch=[pltpu.SemaphoreType.DMA((2,))],
        limit=4,
    )
    if short:
        offsets = (0, 1, 3, 2)
        far = send(pair, lambda z, x, c: (z ^ 2, x, c))
        near = send(pair, lambda z, x, c: (z ^ 1, x, c))
        wrap = send(pair, lambda z, x, c: (z ^ 3, x, c))
        blocks = [pair, near, wrap, far]
    else:
        offsets = (0,)
        blocks = [lax.all_gather(pair, "seq", axis=1, tiled=True)]
    heads = width // HD
    count = 10 if vocab_head.shape[0] % 160 == 0 else 1
    gain = norm_gain.reshape(1, model_width)
    slots, picked, picked_resid, meta, weight, gain, head = call(
        functools.partial(prep_kernel, count),
        (
            jax.ShapeDtypeStruct(scored_slots.shape, jnp.int32),
            jax.ShapeDtypeStruct((samples, heads * cap, HD), BF16),
            jax.ShapeDtypeStruct((rows, model_width), BF16),
            jax.ShapeDtypeStruct((2, lanes), jnp.int32),
            pltpu.VMEM(out_weight.shape, BF16),
            pltpu.VMEM(gain.shape, F32),
            pltpu.VMEM(vocab_head.shape, BF16),
        ),
        [
            keep(array)
            for array in (
                scored_slots, targets, lengths, rewards, queries, residual,
                out_weight, gain, vocab_head,
            )
        ],
        [hbm()] * 9,
        scratch=[
            pltpu.VMEM(targets.shape, jnp.int32),
            pltpu.SMEM(lengths.shape, jnp.int32),
            pltpu.SMEM(rewards.shape, jnp.int32),
            pltpu.VMEM(queries.shape, BF16),
            pltpu.VMEM(residual.shape, BF16),
            pltpu.SemaphoreType.DMA((8 + count,)),
        ],
        limit=12,
    )
    head = pltpu.with_memory_space_constraint(head, pltpu.VMEM)
    weight = pltpu.with_memory_space_constraint(weight, pltpu.VMEM)
    partial_value = call(
        functools.partial(attend_kernel, offsets),
        jax.ShapeDtypeStruct((rows, model_width), BF16),
        [slots, picked, weight, *blocks],
        [vmem()] * (3 + len(blocks)),
    )
    if short:
        other_meta = beside(meta)
        normed, half = call(
            norm_kernel,
            (
                jax.ShapeDtypeStruct((rows, model_width), BF16),
                jax.ShapeDtypeStruct((rows // 2, model_width), BF16),
            ),
            [partial_value, across(partial_value), picked_resid, gain],
            [vmem()] * 4,
        )
        far = send(half, lambda z, x, c: (z ^ 2, x, c))
        split = send(normed, lambda z, x, c: (z ^ (1, 3)[c], x, c))
        side = beside(half)
        split_side = beside(split)
        far_side = beside(far)
        first = column_scores(
            head, meta,
            [normed, split, across(split), far, across(far)],
            [(0, None), ("split", 0), ("split", 1), (2, 0), (2, 1)],
            samples,
        )
        stats = column_scores(
            head, other_meta,
            [side, across(side), split_side, across(split_side), far_side, across(far_side)],
            [(0, 0), (0, 1), ("split", 0), ("split", 1), (2, 0), (2, 1)],
            samples,
            before=first,
        )
        stats = lax.all_to_all(stats, CELL, 0, 0, tiled=True)

        return close(stats, [meta, other_meta], True, samples, cap, length)
    summed = lax.psum(partial_value, "vocab")
    normed = call(
        lambda a, b, r, g, out: norm_kernel(a, b, r, g, out, None),
        jax.ShapeDtypeStruct((rows, model_width), BF16),
        [summed, jnp.zeros_like(summed), picked_resid, gain],
        [vmem()] * 4,
    )
    every = lax.all_gather(normed.reshape(samples, cap, model_width), "seq", axis=1, tiled=True)
    every = lax.all_gather(every, "sample", axis=0, tiled=True).reshape(-1, model_width)
    metas = lax.all_gather(meta, "sample", axis=0)
    stats = tiled_scores(head, every, metas[:, 0, :].reshape(1, -1))
    top = lax.pmax(stats[0], CELL)
    total, pick = lax.psum((jnp.exp(stats[0] - top), stats[1]), CELL)
    stats = jnp.stack([top + jnp.log(total), pick]).reshape(2, sample_size, lanes)
    stats = stats.transpose(1, 0, 2).reshape(1, sample_size * 2, lanes)
    metas = [metas[k] for k in range(sample_size)]
    return close(stats, metas, False, samples, cap, length)


def solution(mesh):
    in_specs = (
        P(("groups", "sample"), "seq", "vocab"),
        P(("groups", "sample"), "seq", "vocab"),
        P(("groups", "sample"), "seq", "vocab"),
        P(("groups", "sample"), "seq", None),
        P("vocab", None),
        P(),
        P(("seq", "sample", "vocab"), None),
        P(("groups", "sample"), None),
        P(("groups", "sample"), None),
        P(("groups", "sample")),
        P(("groups", "sample")),
    )
    out_specs = (
        P(("groups", "sample"), "seq"),
        P(("groups", "sample")),
        P(("groups", "sample")),
        P("groups"),
    )
    return jax.shard_map(shards, mesh=mesh, in_specs=in_specs, out_specs=out_specs, check_vma=False)
```

```python
import functools

import jax
import jax.numpy as jnp
from jax import lax
from jax.experimental import pallas as pl
from jax.experimental.pallas import tpu as pltpu
from jax.sharding import PartitionSpec as P


HD = 128
F32 = jnp.float32
BF16 = jnp.bfloat16
FLOOR = -1e30
CELL = ("seq", "sample", "vocab")


def vmem():
    return pl.BlockSpec(memory_space=pltpu.VMEM)


def hbm():
    return pl.BlockSpec(memory_space=pltpu.HBM)


def keep(array):
    return pltpu.with_memory_space_constraint(array, pltpu.HBM)


def smem():
    return pl.BlockSpec(memory_space=pltpu.SMEM)


def call(body, outs, ins, in_specs, out_specs=None, scratch=(), limit=12, flops=None):
    cost = None
    if flops is not None:
        cost = pl.CostEstimate(flops=flops, bytes_accessed=0, transcendentals=0)
    return pl.pallas_call(
        body,
        cost_estimate=cost,
        out_shape=outs,
        in_specs=in_specs,
        out_specs=jax.tree.map(lambda _: vmem(), outs) if out_specs is None else out_specs,
        scratch_shapes=list(scratch),
        compiler_params=pltpu.CompilerParams(vmem_limit_bytes=limit * 2**20),
    )(*ins)


def iota(shape, dim):
    return lax.broadcasted_iota(jnp.int32, shape, dim)


def own_slot_column(slots_row, seq_at, cap):
    total = slots_row.shape[1]
    hit = iota((cap, total), 1) == iota((cap, total), 0) + seq_at * cap
    return jnp.sum(jnp.where(hit, slots_row, 0), axis=1, keepdims=True)


def pack_kernel(keys, values, out, sems):
    width = keys.shape[2]
    copies = [
        pltpu.make_async_copy(ref, out.at[:, :, pl.ds(n * width, width)], sems.at[n])
        for n, ref in enumerate((keys, values))
    ]
    for copy in copies:
        copy.start()
    for copy in copies:
        copy.wait()


def prep_kernel(
    count, slots_in, targets_in, lengths_in, rewards_in, queries, residual, weight, gain, head,
    slots, q_out, r_out, meta_out, weight_out, gain_out, head_out,
    targets, lengths, rewards, q_in, r_in, sems,
):
    samples, block, width = queries.shape
    total, length = slots.shape[1], targets.shape[1]
    heads = width // HD
    cap = r_out.shape[0] // samples
    seq_at = lax.axis_index("seq")
    lanes = meta_out.shape[1]
    step = head.shape[0] // count
    moves = [
        (slots_in, slots), (targets_in, targets), (lengths_in, lengths), (rewards_in, rewards),
        (queries, q_in), (residual, r_in), (weight, weight_out), (gain, gain_out),
    ]
    for n in range(count):
        moves.append((head.at[pl.ds(n * step, step), :], head_out.at[pl.ds(n * step, step), :]))
    copies = [pltpu.make_async_copy(a, b, sems.at[n]) for n, (a, b) in enumerate(moves)]
    for copy in copies:
        copy.start()
    for copy in copies[:4]:
        copy.wait()
    reward_row = jnp.zeros((1, lanes), jnp.int32)
    onehots = []
    for i in range(samples):
        row = slots[i : i + 1, :]
        local = jnp.clip(own_slot_column(row, seq_at, cap) - seq_at * block, 0, block - 1)
        onehots.append((iota((cap, block), 1) == local).astype(F32).astype(BF16))
        eye = iota((total, total), 0) == iota((total, total), 1)
        column = jnp.sum(jnp.where(eye, jnp.maximum(row, 0), 0), axis=1, keepdims=True)
        spot = iota((total, length), 1) == column
        found = jnp.sum(jnp.where(spot, targets[i : i + 1, :], 0), axis=1, keepdims=True)
        wanted = jnp.sum(jnp.where(eye, found, 0), axis=0, keepdims=True)
        wanted = jnp.where((row >= 0) & (row < lengths[i]), wanted, -1)
        for n in range(total // cap):
            meta_out[n : n + 1, i * cap : (i + 1) * cap] = wanted[:, n * cap : (n + 1) * cap]
        reward_row = jnp.where(iota((1, lanes), 1) == i, rewards[i], reward_row)
    meta_out[total // cap : total // cap + 1, :] = reward_row
    copies[4].wait()
    for i in range(samples):
        picked = jnp.dot(onehots[i], q_in[i], preferred_element_type=F32).astype(BF16)
        for h in range(heads):
            q_out[i, h * cap : (h + 1) * cap, :] = picked[:, h * HD : (h + 1) * HD]
    copies[5].wait()
    for i in range(samples):
        r_out[i * cap : (i + 1) * cap, :] = jnp.dot(
            onehots[i], r_in[i], preferred_element_type=F32
        ).astype(BF16)
    for copy in copies[6:]:
        copy.wait()


def attend_kernel(offsets, slots, queries, weight, *refs):
    blocks, out = refs[:-1], refs[-1]
    samples, stacked, _ = queries.shape
    block_len, kv_width = blocks[0].shape[1], blocks[0].shape[2]
    kv_heads = kv_width // (2 * HD)
    heads = weight.shape[0] // HD
    cap = stacked // heads
    group = heads // kv_heads
    span = block_len * len(blocks)
    seq_at = lax.axis_index("seq")
    lane = iota((1, span), 1)
    key_pos = lane
    if len(blocks) > 1:
        key_pos = jnp.zeros((1, span), jnp.int32)
        for n, flip in enumerate(offsets):
            start = jnp.bitwise_xor(seq_at, flip) * block_len
            key_pos = jnp.where(lane // block_len == n, lane - n * block_len + start, key_pos)
    rows = []
    for i in range(samples):
        column = jnp.maximum(own_slot_column(slots[i : i + 1, :], seq_at, cap), 0)
        reach = jnp.concatenate([column] * group, axis=0)
        allowed = key_pos <= reach
        pieces = []
        for g in range(kv_heads):
            left, right = g * HD, kv_width // 2 + g * HD
            keys = jnp.concatenate([b[i, :, left : left + HD] for b in blocks], axis=0)
            values = jnp.concatenate([b[i, :, right : right + HD] for b in blocks], axis=0)
            query = queries[i, g * group * cap : (g + 1) * group * cap, :]
            scores = lax.dot_general(
                query, keys, (((1,), (1,)), ((), ())), preferred_element_type=F32
            ) * HD ** (-0.5)
            scores = jnp.where(allowed, scores, FLOOR)
            top = jnp.max(scores, axis=1, keepdims=True)
            weights = jnp.where(allowed, jnp.exp(scores - top), 0.0)
            total = jnp.sum(weights, axis=1, keepdims=True)
            mixed = jnp.dot(weights.astype(BF16), values, preferred_element_type=F32)
            mixed = (mixed / total).astype(BF16)
            pieces += [mixed[h * cap : (h + 1) * cap, :] for h in range(group)]
        rows.append(jnp.concatenate(pieces, axis=1))
    attended = jnp.concatenate(rows, axis=0)
    out[...] = jnp.dot(attended, weight[...], preferred_element_type=F32).astype(BF16)


def norm_kernel(mine, other, residual, gain, full, half):
    hidden = residual[...].astype(F32) + (mine[...].astype(F32) + other[...].astype(F32))
    power = jnp.mean(hidden * hidden, axis=-1, keepdims=True)
    full[...] = (hidden * lax.rsqrt(power + 1e-06) * gain[...]).astype(BF16)
    if half is not None:
        count = half.shape[0]
        start = pl.multiple_of(lax.axis_index("vocab") * count, count)
        half[...] = full[pl.ds(start, count), :]


def fold(logits, wanted, first_row, top_ref, sum_ref, pick_ref):
    count, width = logits.shape
    tiles = logits.reshape(count // 8, 8, width)
    old = top_ref[...]
    new = jnp.maximum(old, jnp.max(tiles, axis=0))
    grown = jnp.sum(jnp.exp(tiles - new[None]), axis=0)
    sum_ref[...] = sum_ref[...] * jnp.exp(old - new) + grown
    top_ref[...] = new
    rows = iota(tiles.shape, 0) * 8 + iota(tiles.shape, 1)
    hit = rows == (wanted - first_row)[None]
    pick_ref[...] += jnp.sum(jnp.where(hit, tiles, 0.0), axis=0)


def score_tile(head, states, wanted, buffers, top_ref, sum_ref, pick_ref, step, unroll, base):
    top_ref[...] = jnp.full(top_ref.shape, FLOOR, F32)
    sum_ref[...] = jnp.zeros(sum_ref.shape, F32)
    pick_ref[...] = jnp.zeros(pick_ref.shape, F32)
    buffers[1][...] = jnp.full(buffers[1].shape, FLOOR, F32)
    local = wanted - base
    local = jnp.where((local >= 0) & (local < head.shape[0]), local, -(1 << 30))
    local = jnp.broadcast_to(local, top_ref.shape)

    def body(at, carry):
        for j in range(unroll):
            first = at * (unroll * step) + j * step
            block = head[pl.ds(pl.multiple_of(first, step), step), :]
            logits = lax.dot_general(
                block, states[...], (((1,), (1,)), ((), ())), preferred_element_type=F32
            )
            fold(buffers[(j + 1) % 2][...], local, first - step, top_ref, sum_ref, pick_ref)
            buffers[j % 2][...] = logits
        return carry

    total = head.shape[0]
    lax.fori_loop(0, total // (unroll * step), body, 0)
    fold(buffers[(unroll - 1) % 2][...], local, total - step, top_ref, sum_ref, pick_ref)
    top = jnp.max(top_ref[...], axis=0, keepdims=True)
    scale = jnp.exp(top_ref[...] - top)
    total = jnp.sum(sum_ref[...] * scale, axis=0, keepdims=True)
    return top + jnp.log(total), jnp.sum(pick_ref[...], axis=0, keepdims=True)


def vocab_base(shard_rows):
    owner = lax.axis_index("seq") * lax.axis_size("sample") + lax.axis_index("sample")
    return (owner * lax.axis_size("vocab") + lax.axis_index("vocab")) * shard_rows


def steps_of(shard_rows):
    for step in (256, 128, 64, 32, 16, 8):
        if shard_rows % (2 * step) == 0:
            unroll = 10 if shard_rows % (10 * step) == 0 else 2
            return step, unroll
    raise ValueError("head rows")


def column_kernel(places, step, unroll, last, head, meta, other_meta, *refs):
    before, refs = (refs[0], refs[1:]) if last is not None else (None, refs)
    inputs, refs = refs[: sum(place[2] for place in places)], refs[sum(place[2] for place in places) :]
    out, states, buf_a, buf_b, top_ref, sum_ref, pick_ref = refs[:7]
    rows = meta.shape[1]
    seq_at, core = lax.axis_index("seq"), lax.axis_index("vocab")
    wanted = []
    for n, place in enumerate(places):
        held = inputs[: place[2]]
        inputs = inputs[place[2] :]
        for part, ref in enumerate(held):
            count = ref.shape[0]
            start = n * rows
            if len(held) > 1:
                start = pl.multiple_of(start + jnp.bitwise_xor(core, part) * count, count)
            states[pl.ds(start, count), :] = ref[...]
        source = other_meta if place[0] else meta
        wanted.append(source[pl.ds(chip_of(place, seq_at, core), 1), :])
    logs, picks = score_tile(
        head, states, jnp.concatenate(wanted, axis=1), (buf_a, buf_b), top_ref, sum_ref, pick_ref,
        step, unroll, vocab_base(head.shape[0]),
    )
    results = [
        jnp.concatenate([logs[:, n * rows : (n + 1) * rows], picks[:, n * rows : (n + 1) * rows]], axis=1)
        for n in range(len(places))
    ]
    if last is None:
        for n, result in enumerate(results):
            out[n : n + 1, :] = result
        return
    message = refs[7]
    results = [before[n : n + 1, :] for n in range(len(last))] + results
    for place, result in zip([*last, *places], results):
        column = jnp.bitwise_xor(lax.axis_index("sample"), place[0])
        message[pl.ds(column * lax.axis_size("seq") + chip_of(place, seq_at, core), 1), :] = result
    out[...] = jnp.broadcast_to(message[...][None], out.shape)


def chip_of(place, seq_at, core):
    flip = place[1]
    if isinstance(flip, tuple):
        flip = jnp.where(core == 0, flip[0], flip[1])
    return jnp.bitwise_xor(seq_at, flip)


def column_scores(head, meta, other_meta, places, blocks, last=None, before=None):
    step, unroll = steps_of(head.shape[0])
    rows = meta.shape[1]
    total = rows * len(places)
    peers = 1
    for axis in CELL:
        peers *= lax.axis_size(axis)
    chips = peers // lax.axis_size("vocab")
    shape = (len(places), 2 * rows) if last is None else (peers, chips, 2 * rows)
    extra = [] if last is None else [before]
    return call(
        functools.partial(column_kernel, places, step, unroll, last),
        jax.ShapeDtypeStruct(shape, F32),
        [head, meta, other_meta, *extra, *blocks],
        [vmem()] * (3 + len(extra) + len(blocks)),
        scratch=[pltpu.VMEM((total, head.shape[1]), BF16)]
        + [pltpu.VMEM((step, total), F32)] * 2
        + [pltpu.VMEM((8, total), F32)] * 3
        + [pltpu.VMEM((chips, 2 * rows), F32)],
        flops=2 * total * head.shape[0] * head.shape[1],
    )


def tile_kernel(step, unroll, head, states, wanted, out, buf_a, buf_b, top_ref, sum_ref, pick_ref):
    parts = score_tile(
        head, states, wanted[...], (buf_a, buf_b), top_ref, sum_ref, pick_ref,
        step, unroll, vocab_base(head.shape[0]),
    )
    out[...] = jnp.concatenate(parts, axis=0)


def tiled_scores(head, states, wanted):
    step, unroll = steps_of(head.shape[0])
    count, width = states.shape
    tile = next(n for n in (256, 128, count) if count % n == 0)
    return pl.pallas_call(
        functools.partial(tile_kernel, step, unroll),
        grid=(count // tile,),
        out_shape=jax.ShapeDtypeStruct((2, count), F32),
        in_specs=[
            pl.BlockSpec(head.shape, lambda i: (0, 0)),
            pl.BlockSpec((tile, width), lambda i: (i, 0)),
            pl.BlockSpec((1, tile), lambda i: (0, i)),
        ],
        out_specs=pl.BlockSpec((2, tile), lambda i: (0, i)),
        scratch_shapes=[pltpu.VMEM((step, tile), F32)] * 2 + [pltpu.VMEM((8, tile), F32)] * 3,
        compiler_params=pltpu.CompilerParams(
            dimension_semantics=("arbitrary",), vmem_limit_bytes=52 * 2**20
        ),
    )(head, states, wanted)


def close_kernel(relative, columns, length, stats, *refs):
    metas, (tokens_out, scores_out, advantages_out, objective_out, tokens) = refs[:-5], refs[-5:]
    samples, cap = tokens_out.shape
    rows = samples * cap
    chips = tokens.shape[0]
    blocks = chips // columns
    prompts = samples * columns
    where, seq_at = lax.axis_index("sample"), lax.axis_index("seq")
    metas = [ref[...] for ref in metas]
    if relative:
        metas = [jnp.where(where == k, metas[0], metas[1]) for k in range(columns)]
    top = stats[0]
    for s in range(1, stats.shape[0]):
        top = jnp.maximum(top, stats[s])
    total = jnp.exp(stats[0] - top)
    pick = stats[0]
    for s in range(1, stats.shape[0]):
        total += jnp.exp(stats[s] - top)
        pick += stats[s]
    logprob = pick[:, rows:] - (top + jnp.log(total))[:, :rows]
    wanted = jnp.concatenate([meta[:blocks] for meta in metas], axis=0)
    tokens[...] = jnp.where(wanted >= 0, logprob, 0.0)
    paid = [meta[blocks : blocks + 1, :].astype(F32) for meta in metas]
    reward_sum = functools.reduce(lambda a, b: a + b, [jnp.sum(row) for row in paid])
    lane = iota((1, rows), 1)
    objective = jnp.float32(0)
    for k in range(columns):
        summed = jnp.sum(tokens[k * blocks : (k + 1) * blocks, :], axis=0, keepdims=True)
        for i in range(samples):
            score = jnp.sum(summed[:, i * cap : (i + 1) * cap]) / length
            reward = jnp.sum(jnp.where(lane == i, paid[k], 0.0))
            advantage = reward - (reward_sum - reward) / (prompts - 1)
            objective += advantage * score

            @pl.when(where == k)
            def _(score=score, advantage=advantage, i=i):
                scores_out[i] = score
                advantages_out[i] = advantage

    objective_out[0] = -(objective / prompts)
    mine = tokens[pl.ds(where * blocks + seq_at, 1), :]
    for i in range(samples):
        tokens_out[i : i + 1, :] = mine[:, i * cap : (i + 1) * cap]


def close(stats, metas, relative, samples, cap, length):
    columns = lax.axis_size("sample")
    outs = (
        jax.ShapeDtypeStruct((samples, cap), F32),
        jax.ShapeDtypeStruct((samples,), F32),
        jax.ShapeDtypeStruct((samples,), F32),
        jax.ShapeDtypeStruct((1,), F32),
    )
    return call(
        functools.partial(close_kernel, relative, columns, length),
        outs,
        [stats, *metas],
        [vmem()] * (1 + len(metas)),
        out_specs=(vmem(), smem(), smem(), smem()),
        scratch=[pltpu.VMEM((stats.shape[1], samples * cap), F32)],
    )


def steps(
    queries, key_states, value_states, residual, out_weight, norm_gain,
    vocab_head, targets, scored_slots, lengths, rewards,
):
    samples, block, width = queries.shape
    model_width = out_weight.shape[1]
    seq_size, sample_size, vocab_size = (lax.axis_size(axis) for axis in CELL)
    cap = scored_slots.shape[1] // seq_size
    length = targets.shape[1]
    rows = samples * cap
    short = (seq_size, sample_size, vocab_size) == (4, 2, 2) and samples % 2 == 0

    def send(array, target):
        pairs = []
        for z in range(seq_size):
            for x in range(sample_size):
                for c in range(vocab_size):
                    to_z, to_x, to_c = target(z, x, c)
                    source = (z * sample_size + x) * vocab_size + c
                    pairs.append((source, (to_z * sample_size + to_x) * vocab_size + to_c))
        return lax.ppermute(array, CELL, pairs)

    def across(array):
        return send(array, lambda z, x, c: (z, x, c ^ 1))

    def beside(array):
        return send(array, lambda z, x, c: (z, x ^ 1, c))

    kv_shape = (samples, block, 2 * key_states.shape[2])
    pair = call(
        pack_kernel,
        jax.ShapeDtypeStruct(kv_shape, BF16),
        [keep(key_states), keep(value_states)],
        [hbm(), hbm()],
        scratch=[pltpu.SemaphoreType.DMA((2,))],
        limit=4,
    )
    if short:
        offsets = (0, 1, 3, 2)
        far = send(pair, lambda z, x, c: (z ^ 2, x, c))
        near = send(pair, lambda z, x, c: (z ^ 1, x, c))
        wrap = send(pair, lambda z, x, c: (z ^ 3, x, c))
        blocks = [pair, near, wrap, far]
    else:
        offsets = (0,)
        blocks = [lax.all_gather(pair, "seq", axis=1, tiled=True)]
    heads = width // HD
    count = 10 if vocab_head.shape[0] % 160 == 0 else 1
    gain = norm_gain.reshape(1, model_width)
    slots, picked, picked_resid, meta, weight, gain, head = call(
        functools.partial(prep_kernel, count),
        (
            jax.ShapeDtypeStruct(scored_slots.shape, jnp.int32),
            jax.ShapeDtypeStruct((samples, heads * cap, HD), BF16),
            jax.ShapeDtypeStruct((rows, model_width), BF16),
            jax.ShapeDtypeStruct((seq_size + 1, rows), jnp.int32),
            pltpu.VMEM(out_weight.shape, BF16),
            pltpu.VMEM(gain.shape, F32),
            pltpu.VMEM(vocab_head.shape, BF16),
        ),
        [
            keep(array)
            for array in (
                scored_slots, targets, lengths, rewards, queries, residual,
                out_weight, gain, vocab_head,
            )
        ],
        [hbm()] * 9,
        scratch=[
            pltpu.VMEM(targets.shape, jnp.int32),
            pltpu.SMEM(lengths.shape, jnp.int32),
            pltpu.SMEM(rewards.shape, jnp.int32),
            pltpu.VMEM(queries.shape, BF16),
            pltpu.VMEM(residual.shape, BF16),
            pltpu.SemaphoreType.DMA((8 + count,)),
        ],
        limit=12,
    )
    head = pltpu.with_memory_space_constraint(head, pltpu.VMEM)
    weight = pltpu.with_memory_space_constraint(weight, pltpu.VMEM)
    partial_value = call(
        functools.partial(attend_kernel, offsets),
        jax.ShapeDtypeStruct((rows, model_width), BF16),
        [slots, picked, weight, *blocks],
        [vmem()] * (3 + len(blocks)),
    )
    if short:
        other_meta = beside(meta)
        other_partial = across(partial_value)
        normed, half = call(
            norm_kernel,
            (
                jax.ShapeDtypeStruct((rows, model_width), BF16),
                jax.ShapeDtypeStruct((rows // 2, model_width), BF16),
            ),
            [partial_value, other_partial, picked_resid, gain],
            [vmem()] * 4,
        )
        split = send(normed, lambda z, x, c: (z ^ (1, 3)[c], x, c))
        side = beside(half)
        far = send(half, lambda z, x, c: (z ^ 2, x, c))
        split_side = beside(split)
        side_far = send(side, lambda z, x, c: (z ^ 2, x, c))
        split_other = across(split)
        side_other = across(side)
        far_other = across(far)
        split_side_other = across(split_side)
        side_far_other = across(side_far)
        near = [(0, 0, 1), (0, (1, 3), 1), (0, (3, 1), 1), (1, 0, 2)]
        rest = [(0, 2, 2), (1, (1, 3), 1), (1, (3, 1), 1), (1, 2, 2)]
        first = column_scores(
            head, meta, other_meta, near, [normed, split, split_other, side, side_other]
        )
        stats = column_scores(
            head, meta, other_meta, rest,
            [far, far_other, split_side, split_side_other, side_far, side_far_other],
            last=near, before=first,
        )
        stats = lax.all_to_all(stats, CELL, 0, 0, tiled=True)
        return close(stats, [meta, other_meta], True, samples, cap, length)
    summed = lax.psum(partial_value, "vocab")
    normed = call(
        lambda a, b, r, g, out: norm_kernel(a, b, r, g, out, None),
        jax.ShapeDtypeStruct((rows, model_width), BF16),
        [summed, jnp.zeros_like(summed), picked_resid, gain],
        [vmem()] * 4,
    )
    every = lax.all_gather(normed, "seq", axis=0, tiled=True)
    every = lax.all_gather(every, "sample", axis=0, tiled=True)
    metas = lax.all_gather(meta, "sample", axis=0)
    logs, picks = tiled_scores(head, every, metas[:, :seq_size].reshape(1, -1))
    top = lax.pmax(logs, CELL)
    total, pick = lax.psum((jnp.exp(logs - top), picks), CELL)
    logs = (top + jnp.log(total)).reshape(1, -1, rows)
    stats = jnp.concatenate([logs, pick.reshape(1, -1, rows)], axis=2)
    metas = [metas[k] for k in range(sample_size)]
    return close(stats, metas, False, samples, cap, length)


def solution(mesh):
    in_specs = (
        P(("groups", "sample"), "seq", "vocab"),
        P(("groups", "sample"), "seq", "vocab"),
        P(("groups", "sample"), "seq", "vocab"),
        P(("groups", "sample"), "seq", None),
        P("vocab", None),
        P(),
        P(("seq", "sample", "vocab"), None),
        P(("groups", "sample"), None),
        P(("groups", "sample"), None),
        P(("groups", "sample")),
        P(("groups", "sample")),
    )
    out_specs = (
        P(("groups", "sample"), "seq"),
        P(("groups", "sample")),
        P(("groups", "sample")),
        P("groups"),
    )
    step = jax.shard_map(steps, mesh=mesh, in_specs=in_specs, out_specs=out_specs, check_vma=False)
    if tuple(mesh.shape[axis] for axis in CELL) != (4, 2, 2):
        return step
    return step
```

```python
import functools

import jax
import jax.numpy as jnp
from jax import lax
from jax.experimental import pallas as pl
from jax.experimental.pallas import tpu as pltpu
from jax.sharding import PartitionSpec as P


HD = 128
F32 = jnp.float32
BF16 = jnp.bfloat16
FLOOR = -1e30
CELL = ("seq", "sample", "vocab")


def vmem():
    return pl.BlockSpec(memory_space=pltpu.VMEM)


def hbm():
    return pl.BlockSpec(memory_space=pltpu.HBM)


def keep(array):
    return pltpu.with_memory_space_constraint(array, pltpu.HBM)


def smem():
    return pl.BlockSpec(memory_space=pltpu.SMEM)


def call(body, outs, ins, in_specs, out_specs=None, scratch=(), limit=12, flops=None):
    cost = None
    if flops is not None:
        cost = pl.CostEstimate(flops=flops, bytes_accessed=0, transcendentals=0)
    return pl.pallas_call(
        body,
        cost_estimate=cost,
        out_shape=outs,
        in_specs=in_specs,
        out_specs=jax.tree.map(lambda _: vmem(), outs) if out_specs is None else out_specs,
        scratch_shapes=list(scratch),
        compiler_params=pltpu.CompilerParams(vmem_limit_bytes=limit * 2**20),
    )(*ins)


def iota(shape, dim):
    return lax.broadcasted_iota(jnp.int32, shape, dim)


def own_slot_column(slots_row, seq_at, cap):
    total = slots_row.shape[1]
    hit = iota((cap, total), 1) == iota((cap, total), 0) + seq_at * cap
    return jnp.sum(jnp.where(hit, slots_row, 0), axis=1, keepdims=True)


def pack_kernel(keys, values, out, sems):
    width = keys.shape[2]
    copies = [
        pltpu.make_async_copy(ref, out.at[:, :, pl.ds(n * width, width)], sems.at[n])
        for n, ref in enumerate((keys, values))
    ]
    for copy in copies:
        copy.start()
    for copy in copies:
        copy.wait()


def prep_kernel(
    count, slots_in, targets_in, lengths_in, rewards_in, queries, residual, weight, gain, head,
    slots, q_out, r_out, meta_out, weight_out, gain_out, head_out,
    targets, lengths, rewards, q_in, r_in, sems,
):
    samples, block, width = queries.shape
    total, length = slots.shape[1], targets.shape[1]
    heads = width // HD
    cap = r_out.shape[0] // samples
    seq_at = lax.axis_index("seq")
    lanes = meta_out.shape[1]
    step = head.shape[0] // count
    moves = [
        (slots_in, slots), (targets_in, targets), (lengths_in, lengths), (rewards_in, rewards),
        (queries, q_in), (residual, r_in), (weight, weight_out), (gain, gain_out.at[0]),
    ]
    for n in range(count):
        moves.append((head.at[pl.ds(n * step, step), :], head_out.at[pl.ds(n * step, step), :]))
    copies = [pltpu.make_async_copy(a, b, sems.at[n]) for n, (a, b) in enumerate(moves)]
    for copy in copies:
        copy.start()
    for copy in copies[:4]:
        copy.wait()
    reward_row = jnp.zeros((1, lanes), jnp.int32)
    onehots = []
    for i in range(samples):
        row = slots[i : i + 1, :]
        local = jnp.clip(own_slot_column(row, seq_at, cap) - seq_at * block, 0, block - 1)
        onehots.append((iota((cap, block), 1) == local).astype(F32).astype(BF16))
        eye = iota((total, total), 0) == iota((total, total), 1)
        column = jnp.sum(jnp.where(eye, jnp.maximum(row, 0), 0), axis=1, keepdims=True)
        spot = iota((total, length), 1) == column
        found = jnp.sum(jnp.where(spot, targets[i : i + 1, :], 0), axis=1, keepdims=True)
        wanted = jnp.sum(jnp.where(eye, found, 0), axis=0, keepdims=True)
        wanted = jnp.where((row >= 0) & (row < lengths[i]), wanted, -1)
        for n in range(total // cap):
            meta_out[n : n + 1, i * cap : (i + 1) * cap] = wanted[:, n * cap : (n + 1) * cap]
        reward_row = jnp.where(iota((1, lanes), 1) == i, rewards[i], reward_row)
    meta_out[total // cap : total // cap + 1, :] = reward_row
    copies[4].wait()
    for i in range(samples):
        picked = jnp.dot(onehots[i], q_in[i], preferred_element_type=F32).astype(BF16)
        for h in range(heads):
            q_out[i, h * cap : (h + 1) * cap, :] = picked[:, h * HD : (h + 1) * HD]
    copies[5].wait()
    for i in range(samples):
        r_out[i * cap : (i + 1) * cap, :] = jnp.dot(
            onehots[i], r_in[i], preferred_element_type=F32
        ).astype(BF16)
    for copy in copies[6:]:
        copy.wait()


def attend_kernel(offsets, slots, queries, weight, *refs):
    blocks, out = refs[:-1], refs[-1]
    samples, stacked, _ = queries.shape
    block_len, kv_width = blocks[0].shape[1], blocks[0].shape[2]
    kv_heads = kv_width // (2 * HD)
    heads = weight.shape[0] // HD
    cap = stacked // heads
    group = heads // kv_heads
    span = block_len * len(blocks)
    seq_at = lax.axis_index("seq")
    lane = iota((1, span), 1)
    key_pos = lane
    if len(blocks) > 1:
        key_pos = jnp.zeros((1, span), jnp.int32)
        for n, flip in enumerate(offsets):
            start = jnp.bitwise_xor(seq_at, flip) * block_len
            key_pos = jnp.where(lane // block_len == n, lane - n * block_len + start, key_pos)
    rows = []
    for i in range(samples):
        column = jnp.maximum(own_slot_column(slots[i : i + 1, :], seq_at, cap), 0)
        reach = jnp.concatenate([column] * group, axis=0)
        allowed = key_pos <= reach
        pieces = []
        for g in range(kv_heads):
            left, right = g * HD, kv_width // 2 + g * HD
            keys = jnp.concatenate([b[i, :, left : left + HD] for b in blocks], axis=0)
            values = jnp.concatenate([b[i, :, right : right + HD] for b in blocks], axis=0)
            query = queries[i, g * group * cap : (g + 1) * group * cap, :]
            scores = lax.dot_general(
                query, keys, (((1,), (1,)), ((), ())), preferred_element_type=F32
            ) * HD ** (-0.5)
            scores = jnp.where(allowed, scores, FLOOR)
            top = jnp.max(scores, axis=1, keepdims=True)
            weights = jnp.where(allowed, jnp.exp(scores - top), 0.0)
            total = jnp.sum(weights, axis=1, keepdims=True)
            mixed = jnp.dot(weights.astype(BF16), values, preferred_element_type=F32)
            mixed = (mixed / total).astype(BF16)
            pieces += [mixed[h * cap : (h + 1) * cap, :] for h in range(group)]
        rows.append(jnp.concatenate(pieces, axis=1))
    attended = jnp.concatenate(rows, axis=0)
    out[...] = jnp.dot(attended, weight[...], preferred_element_type=F32).astype(BF16)


def norm_kernel(mine, other, residual, gain, full, half):
    hidden = residual[...].astype(F32) + (mine[...].astype(F32) + other[...].astype(F32))
    power = jnp.mean(hidden * hidden, axis=-1, keepdims=True)
    full[...] = (hidden * lax.rsqrt(power + 1e-06) * gain[...]).astype(BF16)
    if half is not None:
        count = half.shape[0]
        start = pl.multiple_of(lax.axis_index("vocab") * count, count)
        half[...] = full[pl.ds(start, count), :]


def fold(logits, wanted, first_row, top_ref, sum_ref, pick_ref):
    count, width = logits.shape
    tiles = logits.reshape(count // 8, 8, width)
    old = top_ref[...]
    new = jnp.maximum(old, jnp.max(tiles, axis=0))
    grown = jnp.sum(jnp.exp(tiles - new[None]), axis=0)
    sum_ref[...] = sum_ref[...] * jnp.exp(old - new) + grown
    top_ref[...] = new
    rows = iota(tiles.shape, 0) * 8 + iota(tiles.shape, 1)
    hit = rows == (wanted - first_row)[None]
    pick_ref[...] += jnp.sum(jnp.where(hit, tiles, 0.0), axis=0)


def score_tile(head, states, wanted, buffers, top_ref, sum_ref, pick_ref, step, unroll, base):
    top_ref[...] = jnp.full(top_ref.shape, FLOOR, F32)
    sum_ref[...] = jnp.zeros(sum_ref.shape, F32)
    pick_ref[...] = jnp.zeros(pick_ref.shape, F32)
    buffers[1][...] = jnp.full(buffers[1].shape, FLOOR, F32)
    local = wanted - base
    local = jnp.where((local >= 0) & (local < head.shape[0]), local, -(1 << 30))
    local = jnp.broadcast_to(local, top_ref.shape)

    def body(at, carry):
        for j in range(unroll):
            first = at * (unroll * step) + j * step
            block = head[pl.ds(pl.multiple_of(first, step), step), :]
            logits = lax.dot_general(
                block, states[...], (((1,), (1,)), ((), ())), preferred_element_type=F32
            )
            fold(buffers[(j + 1) % 2][...], local, first - step, top_ref, sum_ref, pick_ref)
            buffers[j % 2][...] = logits
        return carry

    total = head.shape[0]
    lax.fori_loop(0, total // (unroll * step), body, 0)
    fold(buffers[(unroll - 1) % 2][...], local, total - step, top_ref, sum_ref, pick_ref)
    top = jnp.max(top_ref[...], axis=0, keepdims=True)
    scale = jnp.exp(top_ref[...] - top)
    total = jnp.sum(sum_ref[...] * scale, axis=0, keepdims=True)
    return top + jnp.log(total), jnp.sum(pick_ref[...], axis=0, keepdims=True)


def vocab_base(shard_rows):
    owner = lax.axis_index("seq") * lax.axis_size("sample") + lax.axis_index("sample")
    return (owner * lax.axis_size("vocab") + lax.axis_index("vocab")) * shard_rows


def steps_of(shard_rows):
    for step in (256, 128, 64, 32, 16, 8):
        if shard_rows % (2 * step) == 0:
            unroll = next(n for n in (20, 10, 4, 2) if shard_rows % (n * step) == 0)
            return step, unroll
    raise ValueError("head rows")


def column_kernel(places, step, unroll, last, head, meta, other_meta, *refs):
    before, refs = (refs[0], refs[1:]) if last is not None else (None, refs)
    count = sum(abs(place[2]) for place in places)
    inputs, refs = refs[:count], refs[count:]
    out, states, buf_a, buf_b, top_ref, sum_ref, pick_ref = refs[:7]
    rows = meta.shape[1]
    seq_at, core = lax.axis_index("seq"), lax.axis_index("vocab")
    wanted = []
    for n, place in enumerate(places):
        held = inputs[: abs(place[2])]
        inputs = inputs[abs(place[2]) :]
        if place[2] < 0:
            for part, ref in enumerate(held):

                @pl.when(core == 1 - part)
                def _(ref=ref, n=n):
                    states[n * rows : (n + 1) * rows, :] = ref[...]
        else:
            for part, ref in enumerate(held):
                count = ref.shape[0]
                start = n * rows
                if len(held) > 1:
                    start = pl.multiple_of(start + jnp.bitwise_xor(core, part) * count, count)
                states[pl.ds(start, count), :] = ref[...]
        row = pl.ds(chip_of(place[1], seq_at, core), 1)
        column = of_core(place[0], core)
        wanted.append(jnp.where(column == 1, other_meta[row, :], meta[row, :]))
    logs, picks = score_tile(
        head, states, jnp.concatenate(wanted, axis=1), (buf_a, buf_b), top_ref, sum_ref, pick_ref,
        step, unroll, vocab_base(head.shape[0]),
    )
    results = [
        jnp.concatenate([logs[:, n * rows : (n + 1) * rows], picks[:, n * rows : (n + 1) * rows]], axis=1)
        for n in range(len(places))
    ]
    if last is None:
        for n, result in enumerate(results):
            out[n : n + 1, :] = result
        return
    message = refs[7]
    results = [before[n : n + 1, :] for n in range(len(last))] + results
    for place, result in zip([*last, *places], results):
        column = jnp.bitwise_xor(lax.axis_index("sample"), of_core(place[0], core))
        row = column * lax.axis_size("seq") + chip_of(place[1], seq_at, core)
        message[pl.ds(row, 1), :] = result
    out[...] = jnp.broadcast_to(message[...][None], out.shape)


def of_core(choice, core):
    return jnp.where(core == 0, *choice) if isinstance(choice, tuple) else choice


def chip_of(flip, seq_at, core):
    return jnp.bitwise_xor(seq_at, of_core(flip, core))


def column_scores(head, meta, other_meta, places, blocks, last=None, before=None):
    step, unroll = steps_of(head.shape[0])
    rows = meta.shape[1]
    total = rows * len(places)
    peers = 1
    for axis in CELL:
        peers *= lax.axis_size(axis)
    chips = peers // lax.axis_size("vocab")
    shape = (len(places), 2 * rows) if last is None else (peers, chips, 2 * rows)
    extra = [] if last is None else [before]
    return call(
        functools.partial(column_kernel, places, step, unroll, last),
        jax.ShapeDtypeStruct(shape, F32),
        [head, meta, other_meta, *extra, *blocks],
        [vmem()] * (3 + len(extra) + len(blocks)),
        scratch=[pltpu.VMEM((total, head.shape[1]), BF16)]
        + [pltpu.VMEM((step, total), F32)] * 2
        + [pltpu.VMEM((8, total), F32)] * 3
        + [pltpu.VMEM((chips, 2 * rows), F32)],
        flops=2 * total * head.shape[0] * head.shape[1],
    )


def tile_kernel(step, unroll, head, states, wanted, out, buf_a, buf_b, top_ref, sum_ref, pick_ref):
    parts = score_tile(
        head, states, wanted[...], (buf_a, buf_b), top_ref, sum_ref, pick_ref,
        step, unroll, vocab_base(head.shape[0]),
    )
    out[...] = jnp.concatenate(parts, axis=0)


def tiled_scores(head, states, wanted):
    step, unroll = steps_of(head.shape[0])
    count, width = states.shape
    tile = next(n for n in (256, 128, count) if count % n == 0)
    return pl.pallas_call(
        functools.partial(tile_kernel, step, unroll),
        grid=(count // tile,),
        out_shape=jax.ShapeDtypeStruct((2, count), F32),
        in_specs=[
            pl.BlockSpec(head.shape, lambda i: (0, 0)),
            pl.BlockSpec((tile, width), lambda i: (i, 0)),
            pl.BlockSpec((1, tile), lambda i: (0, i)),
        ],
        out_specs=pl.BlockSpec((2, tile), lambda i: (0, i)),
        scratch_shapes=[pltpu.VMEM((step, tile), F32)] * 2 + [pltpu.VMEM((8, tile), F32)] * 3,
        compiler_params=pltpu.CompilerParams(
            dimension_semantics=("arbitrary",), vmem_limit_bytes=52 * 2**20
        ),
    )(head, states, wanted)


def close_kernel(relative, columns, length, stats, *refs):
    metas, (tokens_out, scores_out, advantages_out, objective_out, tokens) = refs[:-5], refs[-5:]
    samples, cap = tokens_out.shape
    rows = samples * cap
    chips = tokens.shape[0]
    blocks = chips // columns
    prompts = samples * columns
    where, seq_at = lax.axis_index("sample"), lax.axis_index("seq")
    metas = [ref[...] for ref in metas]
    if relative:
        metas = [jnp.where(where == k, metas[0], metas[1]) for k in range(columns)]
    top = stats[0]
    for s in range(1, stats.shape[0]):
        top = jnp.maximum(top, stats[s])
    total = jnp.exp(stats[0] - top)
    pick = stats[0]
    for s in range(1, stats.shape[0]):
        total += jnp.exp(stats[s] - top)
        pick += stats[s]
    logprob = pick[:, rows:] - (top + jnp.log(total))[:, :rows]
    wanted = jnp.concatenate([meta[:blocks] for meta in metas], axis=0)
    tokens[...] = jnp.where(wanted >= 0, logprob, 0.0)
    paid = [meta[blocks : blocks + 1, :].astype(F32) for meta in metas]
    reward_sum = functools.reduce(lambda a, b: a + b, [jnp.sum(row) for row in paid])
    lane = iota((1, rows), 1)
    objective = jnp.float32(0)
    for k in range(columns):
        summed = jnp.sum(tokens[k * blocks : (k + 1) * blocks, :], axis=0, keepdims=True)
        for i in range(samples):
            score = jnp.sum(summed[:, i * cap : (i + 1) * cap]) / length
            reward = jnp.sum(jnp.where(lane == i, paid[k], 0.0))
            advantage = reward - (reward_sum - reward) / (prompts - 1)
            objective += advantage * score

            @pl.when(where == k)
            def _(score=score, advantage=advantage, i=i):
                scores_out[i] = score
                advantages_out[i] = advantage

    objective_out[0] = -(objective / prompts)
    mine = tokens[pl.ds(where * blocks + seq_at, 1), :]
    for i in range(samples):
        tokens_out[i : i + 1, :] = mine[:, i * cap : (i + 1) * cap]


def close(stats, metas, relative, samples, cap, length):
    columns = lax.axis_size("sample")
    outs = (
        jax.ShapeDtypeStruct((samples, cap), F32),
        jax.ShapeDtypeStruct((samples,), F32),
        jax.ShapeDtypeStruct((samples,), F32),
        jax.ShapeDtypeStruct((1,), F32),
    )
    return call(
        functools.partial(close_kernel, relative, columns, length),
        outs,
        [stats, *metas],
        [vmem()] * (1 + len(metas)),
        out_specs=(vmem(), smem(), smem(), smem()),
        scratch=[pltpu.VMEM((stats.shape[1], samples * cap), F32)],
    )


def steps(
    queries, key_states, value_states, residual, out_weight, norm_gain,
    vocab_head, targets, scored_slots, lengths, rewards,
):
    samples, block, width = queries.shape
    model_width = out_weight.shape[1]
    seq_size, sample_size, vocab_size = (lax.axis_size(axis) for axis in CELL)
    cap = scored_slots.shape[1] // seq_size
    length = targets.shape[1]
    rows = samples * cap
    sizes = tuple(lax.axis_size(axis) for axis in ("groups",) + CELL)
    short = sizes == (2, 4, 2, 2) and samples % 2 == 0

    def send(array, target):
        pairs = []
        for z in range(seq_size):
            for x in range(sample_size):
                for c in range(vocab_size):
                    place = target(z, x, c)
                    if place is not None:
                        source = (z * sample_size + x) * vocab_size + c
                        to = (place[0] * sample_size + place[1]) * vocab_size + place[2]
                        pairs.append((source, to))
        return lax.ppermute(array, CELL, pairs)

    def aside(array):
        pairs = []
        for g in range(2):
            for z in range(seq_size):
                for x in range(sample_size):
                    at = ((g * seq_size + z) * sample_size + x) * vocab_size
                    pairs.append((at, (((1 - g) * seq_size + z) * sample_size + x) * vocab_size))
                    pairs.append((at + 1, ((g * seq_size + z) * sample_size + 1 - x) * vocab_size + 1))
        return lax.ppermute(array, ("groups",) + CELL, pairs)

    def across(array):
        return send(array, lambda z, x, c: (z, x, c ^ 1))

    def beside(array):
        return send(array, lambda z, x, c: (z, x ^ 1, c))

    kv_shape = (samples, block, 2 * key_states.shape[2])
    pair = call(
        pack_kernel,
        jax.ShapeDtypeStruct(kv_shape, BF16),
        [keep(key_states), keep(value_states)],
        [hbm(), hbm()],
        scratch=[pltpu.SemaphoreType.DMA((2,))],
        limit=4,
    )
    if short:
        offsets = (0, 1, 3, 2)
        far = send(pair, lambda z, x, c: (z ^ 2, x, c))
        near = send(pair, lambda z, x, c: (z ^ 1, x, c))
        wrap = send(pair, lambda z, x, c: (z ^ 3, x, c))
        blocks = [pair, near, wrap, far]
    else:
        offsets = (0,)
        blocks = [lax.all_gather(pair, "seq", axis=1, tiled=True)]
    heads = width // HD
    count = 10 if vocab_head.shape[0] % 160 == 0 else 1
    slots, picked, picked_resid, meta, weight, gain, head = call(
        functools.partial(prep_kernel, count),
        (
            jax.ShapeDtypeStruct(scored_slots.shape, jnp.int32),
            jax.ShapeDtypeStruct((samples, heads * cap, HD), BF16),
            jax.ShapeDtypeStruct((rows, model_width), BF16),
            jax.ShapeDtypeStruct((seq_size + 1, rows), jnp.int32),
            pltpu.VMEM(out_weight.shape, BF16),
            pltpu.VMEM((1, model_width), F32),
            pltpu.VMEM(vocab_head.shape, BF16),
        ),
        [
            keep(array)
            for array in (
                scored_slots, targets, lengths, rewards, queries, residual,
                out_weight, norm_gain, vocab_head,
            )
        ],
        [hbm()] * 9,
        scratch=[
            pltpu.VMEM(targets.shape, jnp.int32),
            pltpu.SMEM(lengths.shape, jnp.int32),
            pltpu.SMEM(rewards.shape, jnp.int32),
            pltpu.VMEM(queries.shape, BF16),
            pltpu.VMEM(residual.shape, BF16),
            pltpu.SemaphoreType.DMA((8 + count,)),
        ],
        limit=12,
    )
    head = pltpu.with_memory_space_constraint(head, pltpu.VMEM)
    weight = pltpu.with_memory_space_constraint(weight, pltpu.VMEM)
    partial_value = call(
        functools.partial(attend_kernel, offsets),
        jax.ShapeDtypeStruct((rows, model_width), BF16),
        [slots, picked, weight, *blocks],
        [vmem()] * (3 + len(blocks)),
    )
    if short:
        other_meta = beside(meta)
        other_partial = across(partial_value)
        normed, half = call(
            norm_kernel,
            (
                jax.ShapeDtypeStruct((rows, model_width), BF16),
                jax.ShapeDtypeStruct((rows // 2, model_width), BF16),
            ),
            [partial_value, other_partial, picked_resid, gain],
            [vmem()] * 4,
        )
        split = send(normed, lambda z, x, c: (z ^ (1, 3)[c], x, c))
        side = beside(half)
        turn = send(split, lambda z, x, c: (z, x ^ 1, c) if c == 0 else (z ^ 1, x, c))
        split_side = aside(split)
        side_far = send(side, lambda z, x, c: (z ^ 2, x, c))
        split_other = across(split)
        side_other = across(side)
        turn_other = across(turn)
        split_side_other = across(split_side)
        side_far_other = across(side_far)
        near = [(0, 0, 1), (0, (1, 3), 1), (0, (3, 1), 1), (1, 0, 2)]
        rest = [((1, 0), (1, 2), 1), ((0, 1), (2, 1), 1), (1, 3, -2), (1, 2, 2)]
        first = column_scores(
            head, meta, other_meta, near, [normed, split, split_other, side, side_other]
        )
        stats = column_scores(
            head, meta, other_meta, rest,
            [turn, turn_other, split_side, split_side_other, side_far, side_far_other],
            last=near, before=first,
        )
        stats = lax.all_to_all(stats, CELL, 0, 0, tiled=True)
        return close(stats, [meta, other_meta], True, samples, cap, length)
    summed = lax.psum(partial_value, "vocab")
    normed = call(
        lambda a, b, r, g, out: norm_kernel(a, b, r, g, out, None),
        jax.ShapeDtypeStruct((rows, model_width), BF16),
        [summed, jnp.zeros_like(summed), picked_resid, gain],
        [vmem()] * 4,
    )
    every = lax.all_gather(normed, "seq", axis=0, tiled=True)
    every = lax.all_gather(every, "sample", axis=0, tiled=True)
    metas = lax.all_gather(meta, "sample", axis=0)
    logs, picks = tiled_scores(head, every, metas[:, :seq_size].reshape(1, -1))
    top = lax.pmax(logs, CELL)
    total, pick = lax.psum((jnp.exp(logs - top), picks), CELL)
    logs = (top + jnp.log(total)).reshape(1, -1, rows)
    stats = jnp.concatenate([logs, pick.reshape(1, -1, rows)], axis=2)
    metas = [metas[k] for k in range(sample_size)]
    return close(stats, metas, False, samples, cap, length)


def solution(mesh):
    in_specs = (
        P(("groups", "sample"), "seq", "vocab"),
        P(("groups", "sample"), "seq", "vocab"),
        P(("groups", "sample"), "seq", "vocab"),
        P(("groups", "sample"), "seq", None),
        P("vocab", None),
        P(),
        P(("seq", "sample", "vocab"), None),
        P(("groups", "sample"), None),
        P(("groups", "sample"), None),
        P(("groups", "sample")),
        P(("groups", "sample")),
    )
    out_specs = (
        P(("groups", "sample"), "seq"),
        P(("groups", "sample")),
        P(("groups", "sample")),
        P("groups"),
    )
    step = jax.shard_map(steps, mesh=mesh, in_specs=in_specs, out_specs=out_specs, check_vma=False)
    if tuple(mesh.shape[axis] for axis in ("groups",) + CELL) != (2, 4, 2, 2):
        return step
    return step
```

```python
import functools

import jax
import jax.numpy as jnp
from jax import lax
from jax.experimental import pallas as pl
from jax.experimental.pallas import tpu as pltpu
from jax.sharding import PartitionSpec as P


HD = 128
F32 = jnp.float32
BF16 = jnp.bfloat16
FLOOR = -1e30
CELL = ("seq", "sample", "vocab")


def vmem():
    return pl.BlockSpec(memory_space=pltpu.VMEM)


def hbm():
    return pl.BlockSpec(memory_space=pltpu.HBM)


def keep(array):
    return pltpu.with_memory_space_constraint(array, pltpu.HBM)


def smem():
    return pl.BlockSpec(memory_space=pltpu.SMEM)


def call(body, outs, ins, in_specs, out_specs=None, scratch=(), limit=12, flops=None):
    cost = None
    if flops is not None:
        cost = pl.CostEstimate(flops=flops, bytes_accessed=0, transcendentals=0)
    return pl.pallas_call(
        body,
        cost_estimate=cost,
        out_shape=outs,
        in_specs=in_specs,
        out_specs=jax.tree.map(lambda _: vmem(), outs) if out_specs is None else out_specs,
        scratch_shapes=list(scratch),
        compiler_params=pltpu.CompilerParams(vmem_limit_bytes=limit * 2**20),
    )(*ins)


def iota(shape, dim):
    return lax.broadcasted_iota(jnp.int32, shape, dim)


def own_slot_column(slots_row, seq_at, cap):
    total = slots_row.shape[1]
    hit = iota((cap, total), 1) == iota((cap, total), 0) + seq_at * cap
    return jnp.sum(jnp.where(hit, slots_row, 0), axis=1, keepdims=True)


def pack_kernel(keys, values, out, sems):
    width = keys.shape[2]
    copies = [
        pltpu.make_async_copy(ref, out.at[:, :, pl.ds(n * width, width)], sems.at[n])
        for n, ref in enumerate((keys, values))
    ]
    for copy in copies:
        copy.start()
    for copy in copies:
        copy.wait()


def prep_kernel(
    slots_in, targets_in, lengths_in, rewards_in, queries, residual, weight, gain,
    slots, q_out, r_out, meta_out, weight_out, gain_out,
    targets, lengths, rewards, q_in, r_in, sems,
):
    samples, block, width = queries.shape
    total, length = slots.shape[1], targets.shape[1]
    heads = width // HD
    cap = r_out.shape[0] // samples
    seq_at = lax.axis_index("seq")
    lanes = meta_out.shape[1]
    moves = [
        (slots_in, slots), (targets_in, targets), (lengths_in, lengths), (rewards_in, rewards),
        (queries, q_in), (residual, r_in), (weight, weight_out), (gain, gain_out.at[0]),
    ]
    copies = [pltpu.make_async_copy(a, b, sems.at[n]) for n, (a, b) in enumerate(moves)]
    for copy in copies:
        copy.start()
    for copy in copies[:4]:
        copy.wait()
    reward_row = jnp.zeros((1, lanes), jnp.int32)
    onehots = []
    for i in range(samples):
        row = slots[i : i + 1, :]
        local = jnp.clip(own_slot_column(row, seq_at, cap) - seq_at * block, 0, block - 1)
        onehots.append((iota((cap, block), 1) == local).astype(F32).astype(BF16))
        eye = iota((total, total), 0) == iota((total, total), 1)
        column = jnp.sum(jnp.where(eye, jnp.maximum(row, 0), 0), axis=1, keepdims=True)
        spot = iota((total, length), 1) == column
        found = jnp.sum(jnp.where(spot, targets[i : i + 1, :], 0), axis=1, keepdims=True)
        wanted = jnp.sum(jnp.where(eye, found, 0), axis=0, keepdims=True)
        meta_out[i : i + 1, :] = jnp.where((row >= 0) & (row < lengths[i]), wanted, -1)
        reward_row = jnp.where(iota((1, lanes), 1) == i, rewards[i], reward_row)
    meta_out[samples : samples + 1, :] = reward_row
    copies[4].wait()
    for i in range(samples):
        picked = jnp.dot(onehots[i], q_in[i], preferred_element_type=F32).astype(BF16)
        for h in range(heads):
            q_out[i, h * cap : (h + 1) * cap, :] = picked[:, h * HD : (h + 1) * HD]
    copies[5].wait()
    for i in range(samples):
        r_out[i * cap : (i + 1) * cap, :] = jnp.dot(
            onehots[i], r_in[i], preferred_element_type=F32
        ).astype(BF16)
    for copy in copies[6:]:
        copy.wait()


def attend_kernel(offsets, slots, queries, weight, *refs):
    blocks, out = refs[:-1], refs[-1]
    samples, stacked, _ = queries.shape
    block_len, kv_width = blocks[0].shape[1], blocks[0].shape[2]
    kv_heads = kv_width // (2 * HD)
    heads = weight.shape[0] // HD
    cap = stacked // heads
    group = heads // kv_heads
    span = block_len * len(blocks)
    seq_at = lax.axis_index("seq")
    lane = iota((1, span), 1)
    key_pos = lane
    if len(blocks) > 1:
        key_pos = jnp.zeros((1, span), jnp.int32)
        for n, flip in enumerate(offsets):
            start = jnp.bitwise_xor(seq_at, flip) * block_len
            key_pos = jnp.where(lane // block_len == n, lane - n * block_len + start, key_pos)
    rows = []
    for i in range(samples):
        column = jnp.maximum(own_slot_column(slots[i : i + 1, :], seq_at, cap), 0)
        reach = jnp.concatenate([column] * group, axis=0)
        allowed = key_pos <= reach
        pieces = []
        for g in range(kv_heads):
            left, right = g * HD, kv_width // 2 + g * HD
            keys = jnp.concatenate([b[i, :, left : left + HD] for b in blocks], axis=0)
            values = jnp.concatenate([b[i, :, right : right + HD] for b in blocks], axis=0)
            query = queries[i, g * group * cap : (g + 1) * group * cap, :]
            scores = lax.dot_general(
                query, keys, (((1,), (1,)), ((), ())), preferred_element_type=F32
            ) * HD ** (-0.5)
            scores = jnp.where(allowed, scores, FLOOR)
            top = jnp.max(scores, axis=1, keepdims=True)
            weights = jnp.where(allowed, jnp.exp(scores - top), 0.0)
            total = jnp.sum(weights, axis=1, keepdims=True)
            mixed = jnp.dot(weights.astype(BF16), values, preferred_element_type=F32)
            mixed = (mixed / total).astype(BF16)
            pieces += [mixed[h * cap : (h + 1) * cap, :] for h in range(group)]
        rows.append(jnp.concatenate(pieces, axis=1))
    attended = jnp.concatenate(rows, axis=0)
    out[...] = jnp.dot(attended, weight[...], preferred_element_type=F32).astype(BF16)


def parcel_kernel(flips, slots_in, keys, values, queries, residual, *refs):
    outs, (slots, q_in, r_in, sems) = refs[: len(flips)], refs[len(flips) :]
    samples, block, _ = queries.shape
    half = r_in.shape[2]
    seq_at = lax.axis_index("seq")
    cap = slots.shape[1] // samples
    start = pl.multiple_of(lax.axis_index("vocab") * half, half)
    moves = [
        (slots_in, slots), (queries, q_in), (residual.at[:, :, pl.ds(start, half)], r_in),
    ]
    for out, flip in zip(outs, flips):
        taker = jnp.bitwise_xor(seq_at, flip)
        moves.append((keys.at[taker], out.at[pl.ds(0, block), :]))
        moves.append((values.at[taker], out.at[pl.ds(block, block), :]))
    copies = [pltpu.make_async_copy(a, b, sems.at[n]) for n, (a, b) in enumerate(moves)]
    for copy in copies:
        copy.start()
    copies[0].wait()
    onehots = []
    for flip in flips:
        row = slots[pl.ds(jnp.bitwise_xor(seq_at, flip), 1), :]
        local = jnp.clip(own_slot_column(row, seq_at, cap) - seq_at * block, 0, block - 1)
        onehots.append((iota((cap, block), 1) == local).astype(F32).astype(BF16))
    first = 2 * block
    for copy, held in zip(copies[1:3], (q_in, r_in)):
        copy.wait()
        for out, flip, onehot in zip(outs, flips, onehots):
            source = held[jnp.bitwise_xor(seq_at, flip)]
            picked = jnp.dot(onehot, source, preferred_element_type=F32).astype(BF16)
            for h in range(picked.shape[1] // HD):
                out[first + h * cap : first + (h + 1) * cap, :] = picked[:, h * HD : (h + 1) * HD]
        first += q_in.shape[2] // HD * cap
    for copy in copies[3:]:
        copy.wait()


def completion_kernel(flips, block, slots, weight, *refs):
    parcels, (out, residual, attended) = refs[: len(flips)], refs[len(flips) :]
    heads = weight.shape[0] // HD
    seq_at = lax.axis_index("seq")
    cap = attended.shape[0] // len(flips)
    row = slots[pl.ds(seq_at, 1), :]
    owners = [jnp.bitwise_xor(seq_at, flip) for flip in flips]
    span = block * len(flips)
    lane = iota((1, span), 1)
    key_pos = jnp.zeros((1, span), jnp.int32)
    reach = []
    for n, owner in enumerate(owners):
        key_pos = jnp.where(lane // block == n, lane + (owner - n) * block, key_pos)
        reach += [jnp.maximum(own_slot_column(row, owner, cap), 0)] * heads
    first = 2 * block
    last = first + heads * cap
    keys = jnp.concatenate([p[:block, :] for p in parcels], axis=0)
    values = jnp.concatenate([p[block:first, :] for p in parcels], axis=0)
    query = jnp.concatenate([p[first:last, :] for p in parcels], axis=0)
    scores = lax.dot_general(
        query, keys, (((1,), (1,)), ((), ())), preferred_element_type=F32
    ) * HD ** (-0.5)
    allowed = key_pos <= jnp.concatenate(reach, axis=0)
    scores = jnp.where(allowed, scores, FLOOR)
    top = jnp.max(scores, axis=1, keepdims=True)
    weights = jnp.where(allowed, jnp.exp(scores - top), 0.0)
    total = jnp.sum(weights, axis=1, keepdims=True)
    mixed = jnp.dot(weights.astype(BF16), values, preferred_element_type=F32)
    mixed = (mixed / total).astype(BF16)
    for n, (owner, parcel) in enumerate(zip(owners, parcels)):
        spot = pl.ds(pl.multiple_of(owner * cap, cap), cap)
        begin = n * heads * cap
        attended[spot, :] = jnp.concatenate(
            [mixed[begin + h * cap : begin + (h + 1) * cap, :] for h in range(heads)], axis=1
        )
        count = residual.shape[1] // HD
        residual[spot, :] = jnp.concatenate(
            [parcel[last + h * cap : last + (h + 1) * cap, :] for h in range(count)], axis=1
        )
    out[...] = jnp.dot(attended[...], weight[...], preferred_element_type=F32).astype(BF16)


def pair_norm_kernel(mine, other, half_mine, half_other, gain, full, half):
    low = jnp.concatenate([half_mine[...], half_other[...]], axis=1)
    high = jnp.concatenate([half_other[...], half_mine[...]], axis=1)
    norm_kernel(mine, other, jnp.where(lax.axis_index("vocab") == 0, low, high), gain, full, half)


def norm_kernel(mine, other, residual, gain, full, half):
    hidden = residual[...].astype(F32) + (mine[...].astype(F32) + other[...].astype(F32))
    power = jnp.mean(hidden * hidden, axis=-1, keepdims=True)
    full[...] = (hidden * lax.rsqrt(power + 1e-06) * gain[...]).astype(BF16)
    if half is not None:
        count = half.shape[0]
        start = pl.multiple_of(lax.axis_index("vocab") * count, count)
        half[...] = full[pl.ds(start, count), :]


def fold(logits, wanted, first_row, top_ref, sum_ref, pick_ref):
    count, width = logits.shape
    tiles = logits.reshape(count // 8, 8, width)
    old = top_ref[...]
    new = jnp.maximum(old, jnp.max(tiles, axis=0))
    grown = jnp.sum(jnp.exp(tiles - new[None]), axis=0)
    sum_ref[...] = sum_ref[...] * jnp.exp(old - new) + grown
    top_ref[...] = new
    rows = iota(tiles.shape, 0) * 8 + iota(tiles.shape, 1)
    hit = rows == (wanted - first_row)[None]
    pick_ref[...] += jnp.sum(jnp.where(hit, tiles, 0.0), axis=0)


def score_tile(head, states, wanted, buffers, top_ref, sum_ref, pick_ref, step, unroll, base):
    top_ref[...] = jnp.full(top_ref.shape, FLOOR, F32)
    sum_ref[...] = jnp.zeros(sum_ref.shape, F32)
    pick_ref[...] = jnp.zeros(pick_ref.shape, F32)
    buffers[1][...] = jnp.full(buffers[1].shape, FLOOR, F32)
    local = wanted - base
    local = jnp.where((local >= 0) & (local < head.shape[0]), local, -(1 << 30))
    local = jnp.broadcast_to(local, top_ref.shape)

    def body(at, carry):
        for j in range(unroll):
            first = at * (unroll * step) + j * step
            block = head[pl.ds(pl.multiple_of(first, step), step), :]
            logits = lax.dot_general(
                block, states[...], (((1,), (1,)), ((), ())), preferred_element_type=F32
            )
            fold(buffers[(j + 1) % 2][...], local, first - step, top_ref, sum_ref, pick_ref)
            buffers[j % 2][...] = logits
        return carry

    total = head.shape[0]
    lax.fori_loop(0, total // (unroll * step), body, 0)
    fold(buffers[(unroll - 1) % 2][...], local, total - step, top_ref, sum_ref, pick_ref)
    top = jnp.max(top_ref[...], axis=0, keepdims=True)
    scale = jnp.exp(top_ref[...] - top)
    total = jnp.sum(sum_ref[...] * scale, axis=0, keepdims=True)
    return top + jnp.log(total), jnp.sum(pick_ref[...], axis=0, keepdims=True)


def vocab_base(shard_rows):
    owner = lax.axis_index("seq") * lax.axis_size("sample") + lax.axis_index("sample")
    return (owner * lax.axis_size("vocab") + lax.axis_index("vocab")) * shard_rows


def steps_of(shard_rows):
    for step in (256, 128, 64, 32, 16, 8):
        if shard_rows % (2 * step) == 0:
            unroll = next(n for n in (20, 10, 4, 2) if shard_rows % (n * step) == 0)
            return step, unroll
    raise ValueError("head rows")


def column_kernel(places, step, unroll, last, head, meta, other_meta, *refs):
    before, refs = (refs[0], refs[1:]) if last is not None else (None, refs)
    count = sum(abs(place[2]) for place in places)
    inputs, refs = refs[:count], refs[count:]
    out, states, buf_a, buf_b, top_ref, sum_ref, pick_ref = refs[:7]
    rows = meta.shape[1]
    seq_at, core = lax.axis_index("seq"), lax.axis_index("vocab")
    wanted = []
    for n, place in enumerate(places):
        held = inputs[: abs(place[2])]
        inputs = inputs[abs(place[2]) :]
        if place[2] < 0:
            for part, ref in enumerate(held):

                @pl.when(core == 1 - part)
                def _(ref=ref, n=n):
                    states[n * rows : (n + 1) * rows, :] = ref[...]
        else:
            for part, ref in enumerate(held):
                count = ref.shape[0]
                start = n * rows
                if len(held) > 1:
                    start = pl.multiple_of(start + jnp.bitwise_xor(core, part) * count, count)
                states[pl.ds(start, count), :] = ref[...]
        row = pl.ds(chip_of(place[1], seq_at, core), 1)
        column = of_core(place[0], core)
        wanted.append(jnp.where(column == 1, other_meta[row, :], meta[row, :]))
    logs, picks = score_tile(
        head, states, jnp.concatenate(wanted, axis=1), (buf_a, buf_b), top_ref, sum_ref, pick_ref,
        step, unroll, vocab_base(head.shape[0]),
    )
    results = [
        jnp.concatenate([logs[:, n * rows : (n + 1) * rows], picks[:, n * rows : (n + 1) * rows]], axis=1)
        for n in range(len(places))
    ]
    if last is None:
        for n, result in enumerate(results):
            out[n : n + 1, :] = result
        return
    message = refs[7]
    results = [before[n : n + 1, :] for n in range(len(last))] + results
    for place, result in zip([*last, *places], results):
        column = jnp.bitwise_xor(lax.axis_index("sample"), of_core(place[0], core))
        row = column * lax.axis_size("seq") + chip_of(place[1], seq_at, core)
        message[pl.ds(row, 1), :] = result
    out[...] = jnp.broadcast_to(message[...][None], out.shape)


def of_core(choice, core):
    return jnp.where(core == 0, *choice) if isinstance(choice, tuple) else choice


def chip_of(flip, seq_at, core):
    return jnp.bitwise_xor(seq_at, of_core(flip, core))


def column_scores(head, meta, other_meta, places, blocks, last=None, before=None):
    step, unroll = steps_of(head.shape[0])
    rows = meta.shape[1]
    total = rows * len(places)
    peers = 1
    for axis in CELL:
        peers *= lax.axis_size(axis)
    chips = peers // lax.axis_size("vocab")
    shape = (len(places), 2 * rows) if last is None else (peers, chips, 2 * rows)
    extra = [] if last is None else [before]
    return call(
        functools.partial(column_kernel, places, step, unroll, last),
        jax.ShapeDtypeStruct(shape, F32),
        [head, meta, other_meta, *extra, *blocks],
        [vmem()] * (3 + len(extra) + len(blocks)),
        scratch=[pltpu.VMEM((total, head.shape[1]), BF16)]
        + [pltpu.VMEM((step, total), F32)] * 2
        + [pltpu.VMEM((8, total), F32)] * 3
        + [pltpu.VMEM((chips, 2 * rows), F32)],
        flops=2 * total * head.shape[0] * head.shape[1],
    )


def tile_kernel(step, unroll, head, states, wanted, out, buf_a, buf_b, top_ref, sum_ref, pick_ref):
    parts = score_tile(
        head, states, wanted[...], (buf_a, buf_b), top_ref, sum_ref, pick_ref,
        step, unroll, vocab_base(head.shape[0]),
    )
    out[...] = jnp.concatenate(parts, axis=0)


def tiled_scores(head, states, wanted):
    step, unroll = steps_of(head.shape[0])
    count, width = states.shape
    tile = next(n for n in (256, 128, count) if count % n == 0)
    return pl.pallas_call(
        functools.partial(tile_kernel, step, unroll),
        grid=(count // tile,),
        out_shape=jax.ShapeDtypeStruct((2, count), F32),
        in_specs=[
            pl.BlockSpec(head.shape, lambda i: (0, 0)),
            pl.BlockSpec((tile, width), lambda i: (i, 0)),
            pl.BlockSpec((1, tile), lambda i: (0, i)),
        ],
        out_specs=pl.BlockSpec((2, tile), lambda i: (0, i)),
        scratch_shapes=[pltpu.VMEM((step, tile), F32)] * 2 + [pltpu.VMEM((8, tile), F32)] * 3,
        compiler_params=pltpu.CompilerParams(
            dimension_semantics=("arbitrary",), vmem_limit_bytes=52 * 2**20
        ),
    )(head, states, wanted)


def close_kernel(relative, columns, length, stats, *refs):
    metas, (tokens_out, scores_out, advantages_out, objective_out, tokens) = refs[:-5], refs[-5:]
    samples, cap = tokens_out.shape
    slots = tokens.shape[1]
    prompts = samples * columns
    where, seq_at = lax.axis_index("sample"), lax.axis_index("seq")
    metas = [ref[...] for ref in metas]
    if relative:
        metas = [jnp.where(where == k, metas[0], metas[1]) for k in range(columns)]
    top = stats[0]
    for s in range(1, stats.shape[0]):
        top = jnp.maximum(top, stats[s])
    total = jnp.exp(stats[0] - top)
    pick = stats[0]
    for s in range(1, stats.shape[0]):
        total += jnp.exp(stats[s] - top)
        pick += stats[s]
    logprob = pick[:, slots:] - (top + jnp.log(total))[:, :slots]
    wanted = jnp.concatenate([meta[:samples] for meta in metas], axis=0)
    tokens[...] = jnp.where(wanted >= 0, logprob, 0.0)
    paid = [meta[samples : samples + 1, :].astype(F32) for meta in metas]
    reward_sum = functools.reduce(lambda a, b: a + b, [jnp.sum(row) for row in paid])
    lane = iota((1, slots), 1)
    objective = jnp.float32(0)
    for k in range(columns):
        for i in range(samples):
            at = k * samples + i
            score = jnp.sum(tokens[at : at + 1, :]) / length
            reward = jnp.sum(jnp.where(lane == i, paid[k], 0.0))
            advantage = reward - (reward_sum - reward) / (prompts - 1)
            objective += advantage * score

            @pl.when(where == k)
            def _(score=score, advantage=advantage, i=i):
                scores_out[i] = score
                advantages_out[i] = advantage

    objective_out[0] = -(objective / prompts)
    mine = tokens[:samples, :]
    for k in range(1, columns):
        mine = jnp.where(where == k, tokens[k * samples : (k + 1) * samples, :], mine)
    piece = mine[:, :cap]
    for n in range(1, slots // cap):
        piece = jnp.where(seq_at == n, mine[:, n * cap : (n + 1) * cap], piece)
    tokens_out[...] = piece


def close(stats, metas, relative, samples, cap, length):
    columns = lax.axis_size("sample")
    outs = (
        jax.ShapeDtypeStruct((samples, cap), F32),
        jax.ShapeDtypeStruct((samples,), F32),
        jax.ShapeDtypeStruct((samples,), F32),
        jax.ShapeDtypeStruct((1,), F32),
    )
    return call(
        functools.partial(close_kernel, relative, columns, length),
        outs,
        [stats, *metas],
        [vmem()] * (1 + len(metas)),
        out_specs=(vmem(), smem(), smem(), smem()),
        scratch=[pltpu.VMEM((stats.shape[1], stats.shape[2] // 2), F32)],
    )


def steps(
    queries, key_states, value_states, residual, out_weight, norm_gain,
    vocab_head, targets, scored_slots, lengths, rewards,
):
    samples, block, width = queries.shape
    model_width = out_weight.shape[1]
    seq_size, sample_size, vocab_size = (lax.axis_size(axis) for axis in CELL)
    cap = scored_slots.shape[1] // seq_size
    length = targets.shape[1]
    rows = samples * cap
    sizes = tuple(lax.axis_size(axis) for axis in ("groups",) + CELL)
    short = sizes == (2, 4, 2, 2) and samples == seq_size and key_states.shape[2] == HD

    def send(array, target):
        pairs = []
        for z in range(seq_size):
            for x in range(sample_size):
                for c in range(vocab_size):
                    place = target(z, x, c)
                    if place is not None:
                        source = (z * sample_size + x) * vocab_size + c
                        to = (place[0] * sample_size + place[1]) * vocab_size + place[2]
                        pairs.append((source, to))
        return lax.ppermute(array, CELL, pairs)

    def aside(array):
        pairs = []
        for g in range(2):
            for z in range(seq_size):
                for x in range(sample_size):
                    at = ((g * seq_size + z) * sample_size + x) * vocab_size
                    pairs.append((at, (((1 - g) * seq_size + z) * sample_size + x) * vocab_size))
                    pairs.append((at + 1, ((g * seq_size + z) * sample_size + 1 - x) * vocab_size + 1))
        return lax.ppermute(array, ("groups",) + CELL, pairs)

    def across(array):
        return send(array, lambda z, x, c: (z, x, c ^ 1))

    def beside(array):
        return send(array, lambda z, x, c: (z, x ^ 1, c))

    flips = (0, 2, 3, 1)
    if short:
        half_width = model_width // vocab_size
        parcel_rows = 2 * block + (width + half_width) // HD * cap
        parcels = call(
            functools.partial(parcel_kernel, flips),
            tuple(jax.ShapeDtypeStruct((parcel_rows, HD), BF16) for _ in flips),
            [keep(a) for a in (scored_slots, key_states, value_states, queries, residual)],
            [hbm()] * 5,
            scratch=[
                pltpu.VMEM(scored_slots.shape, jnp.int32),
                pltpu.VMEM(queries.shape, BF16),
                pltpu.VMEM((samples, block, half_width), BF16),
                pltpu.SemaphoreType.DMA((3 + 2 * len(flips),)),
            ],
        )
        far = send(parcels[1], lambda z, x, c: (z ^ 2, x, c))
        wrap = send(parcels[2], lambda z, x, c: (z ^ 3, x, c))
        near = send(parcels[3], lambda z, x, c: (z ^ 1, x, c))
        blocks = [parcels[0], far, wrap, near]
    else:
        offsets = (0,)
        kv_shape = (samples, block, 2 * key_states.shape[2])
        pair = call(
            pack_kernel,
            jax.ShapeDtypeStruct(kv_shape, BF16),
            [keep(key_states), keep(value_states)],
            [hbm(), hbm()],
            scratch=[pltpu.SemaphoreType.DMA((2,))],
            limit=4,
        )
        blocks = [lax.all_gather(pair, "seq", axis=1, tiled=True)]
    heads = width // HD
    slots, picked, picked_resid, meta, weight, gain = call(
        prep_kernel,
        (
            jax.ShapeDtypeStruct(scored_slots.shape, jnp.int32),
            jax.ShapeDtypeStruct((samples, heads * cap, HD), BF16),
            jax.ShapeDtypeStruct((rows, model_width), BF16),
            jax.ShapeDtypeStruct((samples + 1, scored_slots.shape[1]), jnp.int32),
            pltpu.VMEM(out_weight.shape, BF16),
            pltpu.VMEM((1, model_width), F32),
        ),
        [
            keep(array)
            for array in (
                scored_slots, targets, lengths, rewards, queries, residual,
                out_weight, norm_gain,
            )
        ],
        [hbm()] * 8,
        scratch=[
            pltpu.VMEM(targets.shape, jnp.int32),
            pltpu.SMEM(lengths.shape, jnp.int32),
            pltpu.SMEM(rewards.shape, jnp.int32),
            pltpu.VMEM(queries.shape, BF16),
            pltpu.VMEM(residual.shape, BF16),
            pltpu.SemaphoreType.DMA((8,)),
        ],
        limit=12,
    )
    head = pltpu.with_memory_space_constraint(vocab_head, pltpu.VMEM)
    weight = pltpu.with_memory_space_constraint(weight, pltpu.VMEM)
    if short:
        partial_value, half_resid = call(
            functools.partial(completion_kernel, flips, block),
            (
                jax.ShapeDtypeStruct((rows, model_width), BF16),
                jax.ShapeDtypeStruct((rows, half_width), BF16),
            ),
            [slots, weight, *blocks],
            [vmem()] * (2 + len(blocks)),
            scratch=[pltpu.VMEM((rows, width), BF16)],
            flops=10**10,
        )
    else:
        partial_value = call(
            functools.partial(attend_kernel, offsets),
            jax.ShapeDtypeStruct((rows, model_width), BF16),
            [slots, picked, weight, *blocks],
            [vmem()] * (3 + len(blocks)),
        )
    if short:
        other_meta = beside(meta)
        other_partial = across(partial_value)
        other_resid = across(half_resid)
        normed, half = call(
            pair_norm_kernel,
            (
                jax.ShapeDtypeStruct((rows, model_width), BF16),
                jax.ShapeDtypeStruct((rows // 2, model_width), BF16),
            ),
            [partial_value, other_partial, half_resid, other_resid, gain],
            [vmem()] * 5,
        )
        split = send(normed, lambda z, x, c: (z ^ (1, 3)[c], x, c))
        side = beside(half)
        turn = send(split, lambda z, x, c: (z, x ^ 1, c) if c == 0 else (z ^ 1, x, c))
        split_side = aside(split)
        side_far = send(side, lambda z, x, c: (z ^ 2, x, c))
        split_other = across(split)
        side_other = across(side)
        turn_other = across(turn)
        split_side_other = across(split_side)
        side_far_other = across(side_far)
        near = [(0, 0, 1), (0, (1, 3), 1), (0, (3, 1), 1), (1, 0, 2)]
        rest = [((1, 0), (1, 2), 1), ((0, 1), (2, 1), 1), (1, 3, -2), (1, 2, 2)]
        first = column_scores(
            head, meta, other_meta, near, [normed, split, split_other, side, side_other]
        )
        stats = column_scores(
            head, meta, other_meta, rest,
            [turn, turn_other, split_side, split_side_other, side_far, side_far_other],
            last=near, before=first,
        )
        stats = lax.all_to_all(stats, CELL, 0, 0, tiled=True)
        return close(stats, [meta, other_meta], True, samples, cap, length)
    summed = lax.psum(partial_value, "vocab")
    normed = call(
        lambda a, b, r, g, out: norm_kernel(a, b, r, g, out, None),
        jax.ShapeDtypeStruct((rows, model_width), BF16),
        [summed, jnp.zeros_like(summed), picked_resid, gain],
        [vmem()] * 4,
    )
    every = lax.all_gather(normed, "seq", axis=0, tiled=True)
    every = lax.all_gather(every, "sample", axis=0, tiled=True)
    metas = lax.all_gather(meta, "sample", axis=0)
    by_chip = (sample_size, samples, seq_size, cap)
    wanted = metas[:, :samples].reshape(by_chip).transpose(0, 2, 1, 3).reshape(1, -1)
    logs, picks = tiled_scores(vocab_head, every, wanted)
    top = lax.pmax(logs, CELL)
    total, pick = lax.psum((jnp.exp(logs - top), picks), CELL)
    by_row = (sample_size, seq_size, samples, cap)
    stats = [
        part.reshape(by_row).transpose(0, 2, 1, 3).reshape(1, sample_size * samples, seq_size * cap)
        for part in (top + jnp.log(total), pick)
    ]
    stats = jnp.concatenate(stats, axis=2)
    metas = [metas[k] for k in range(sample_size)]
    return close(stats, metas, False, samples, cap, length)


def solution(mesh):
    in_specs = (
        P(("groups", "sample"), "seq", "vocab"),
        P(("groups", "sample"), "seq", "vocab"),
        P(("groups", "sample"), "seq", "vocab"),
        P(("groups", "sample"), "seq", None),
        P("vocab", None),
        P(),
        P(("seq", "sample", "vocab"), None),
        P(("groups", "sample"), None),
        P(("groups", "sample"), None),
        P(("groups", "sample")),
        P(("groups", "sample")),
    )
    out_specs = (
        P(("groups", "sample"), "seq"),
        P(("groups", "sample")),
        P(("groups", "sample")),
        P("groups"),
    )
    step = jax.shard_map(steps, mesh=mesh, in_specs=in_specs, out_specs=out_specs, check_vma=False)
    if tuple(mesh.shape[axis] for axis in ("groups",) + CELL) != (2, 4, 2, 2):
        return step
    return step
```

```python
import functools

import jax
import jax.numpy as jnp
from jax import lax
from jax.experimental import pallas as pl
from jax.experimental.pallas import tpu as pltpu
from jax.sharding import PartitionSpec as P


HD = 128
F32 = jnp.float32
BF16 = jnp.bfloat16
FLOOR = -1e30
CELL = ("seq", "sample", "vocab")


def vmem():
    return pl.BlockSpec(memory_space=pltpu.VMEM)


def hbm():
    return pl.BlockSpec(memory_space=pltpu.HBM)


def keep(array):
    return pltpu.with_memory_space_constraint(array, pltpu.HBM)


def smem():
    return pl.BlockSpec(memory_space=pltpu.SMEM)


def call(body, outs, ins, in_specs, out_specs=None, scratch=(), limit=12, flops=None):
    cost = None
    if flops is not None:
        cost = pl.CostEstimate(flops=flops, bytes_accessed=0, transcendentals=0)
    return pl.pallas_call(
        body,
        cost_estimate=cost,
        out_shape=outs,
        in_specs=in_specs,
        out_specs=jax.tree.map(lambda _: vmem(), outs) if out_specs is None else out_specs,
        scratch_shapes=list(scratch),
        compiler_params=pltpu.CompilerParams(vmem_limit_bytes=limit * 2**20),
    )(*ins)


def iota(shape, dim):
    return lax.broadcasted_iota(jnp.int32, shape, dim)


def own_slot_column(slots_row, seq_at, cap):
    total = slots_row.shape[1]
    hit = iota((cap, total), 1) == iota((cap, total), 0) + seq_at * cap
    return jnp.sum(jnp.where(hit, slots_row, 0), axis=1, keepdims=True)


def pack_kernel(keys, values, out, sems):
    width = keys.shape[2]
    copies = [
        pltpu.make_async_copy(ref, out.at[:, :, pl.ds(n * width, width)], sems.at[n])
        for n, ref in enumerate((keys, values))
    ]
    for copy in copies:
        copy.start()
    for copy in copies:
        copy.wait()


def prep_kernel(
    slots_in, targets_in, lengths_in, rewards_in, queries, residual, weight, gain,
    slots, q_out, r_out, meta_out, weight_out, gain_out,
    targets, lengths, rewards, q_in, r_in, sems,
):
    samples, block, width = queries.shape
    total, length = slots.shape[1], targets.shape[1]
    heads = width // HD
    cap = r_out.shape[0] // samples
    seq_at = lax.axis_index("seq")
    lanes = meta_out.shape[1]
    moves = [
        (slots_in, slots), (targets_in, targets), (lengths_in, lengths), (rewards_in, rewards),
        (queries, q_in), (residual, r_in), (weight, weight_out), (gain, gain_out.at[0]),
    ]
    copies = [pltpu.make_async_copy(a, b, sems.at[n]) for n, (a, b) in enumerate(moves)]
    for copy in copies:
        copy.start()
    for copy in copies[:4]:
        copy.wait()
    reward_row = jnp.zeros((1, lanes), jnp.int32)
    onehots = []
    for i in range(samples):
        row = slots[i : i + 1, :]
        local = jnp.clip(own_slot_column(row, seq_at, cap) - seq_at * block, 0, block - 1)
        onehots.append((iota((cap, block), 1) == local).astype(F32).astype(BF16))
        eye = iota((total, total), 0) == iota((total, total), 1)
        column = jnp.sum(jnp.where(eye, jnp.maximum(row, 0), 0), axis=1, keepdims=True)
        spot = iota((total, length), 1) == column
        found = jnp.sum(jnp.where(spot, targets[i : i + 1, :], 0), axis=1, keepdims=True)
        wanted = jnp.sum(jnp.where(eye, found, 0), axis=0, keepdims=True)
        meta_out[i : i + 1, :] = jnp.where((row >= 0) & (row < lengths[i]), wanted, -1)
        reward_row = jnp.where(iota((1, lanes), 1) == i, rewards[i], reward_row)
    meta_out[samples : samples + 1, :] = reward_row
    copies[4].wait()
    for i in range(samples):
        picked = jnp.dot(onehots[i], q_in[i], preferred_element_type=F32).astype(BF16)
        for h in range(heads):
            q_out[i, h * cap : (h + 1) * cap, :] = picked[:, h * HD : (h + 1) * HD]
    copies[5].wait()
    for i in range(samples):
        r_out[i * cap : (i + 1) * cap, :] = jnp.dot(
            onehots[i], r_in[i], preferred_element_type=F32
        ).astype(BF16)
    for copy in copies[6:]:
        copy.wait()


def attend_kernel(offsets, slots, queries, weight, *refs):
    blocks, out = refs[:-1], refs[-1]
    samples, stacked, _ = queries.shape
    block_len, kv_width = blocks[0].shape[1], blocks[0].shape[2]
    kv_heads = kv_width // (2 * HD)
    heads = weight.shape[0] // HD
    cap = stacked // heads
    group = heads // kv_heads
    span = block_len * len(blocks)
    seq_at = lax.axis_index("seq")
    lane = iota((1, span), 1)
    key_pos = lane
    if len(blocks) > 1:
        key_pos = jnp.zeros((1, span), jnp.int32)
        for n, flip in enumerate(offsets):
            start = jnp.bitwise_xor(seq_at, flip) * block_len
            key_pos = jnp.where(lane // block_len == n, lane - n * block_len + start, key_pos)
    rows = []
    for i in range(samples):
        column = jnp.maximum(own_slot_column(slots[i : i + 1, :], seq_at, cap), 0)
        reach = jnp.concatenate([column] * group, axis=0)
        allowed = key_pos <= reach
        pieces = []
        for g in range(kv_heads):
            left, right = g * HD, kv_width // 2 + g * HD
            keys = jnp.concatenate([b[i, :, left : left + HD] for b in blocks], axis=0)
            values = jnp.concatenate([b[i, :, right : right + HD] for b in blocks], axis=0)
            query = queries[i, g * group * cap : (g + 1) * group * cap, :]
            scores = lax.dot_general(
                query, keys, (((1,), (1,)), ((), ())), preferred_element_type=F32
            ) * HD ** (-0.5)
            scores = jnp.where(allowed, scores, FLOOR)
            top = jnp.max(scores, axis=1, keepdims=True)
            weights = jnp.where(allowed, jnp.exp(scores - top), 0.0)
            total = jnp.sum(weights, axis=1, keepdims=True)
            mixed = jnp.dot(weights.astype(BF16), values, preferred_element_type=F32)
            mixed = (mixed / total).astype(BF16)
            pieces += [mixed[h * cap : (h + 1) * cap, :] for h in range(group)]
        rows.append(jnp.concatenate(pieces, axis=1))
    attended = jnp.concatenate(rows, axis=0)
    out[...] = jnp.dot(attended, weight[...], preferred_element_type=F32).astype(BF16)


def parcel_kernel(flips, slots_in, keys, values, queries, residual, *refs):
    outs, (slots, q_in, r_in, sems) = refs[: len(flips)], refs[len(flips) :]
    samples, block, _ = queries.shape
    half = r_in.shape[2]
    seq_at = lax.axis_index("seq")
    cap = slots.shape[1] // samples
    start = pl.multiple_of(lax.axis_index("vocab") * half, half)
    moves = [
        (slots_in, slots), (queries, q_in), (residual.at[:, :, pl.ds(start, half)], r_in),
    ]
    for out, flip in zip(outs, flips):
        taker = jnp.bitwise_xor(seq_at, flip)
        moves.append((keys.at[taker], out.at[pl.ds(0, block), :]))
        moves.append((values.at[taker], out.at[pl.ds(block, block), :]))
    copies = [pltpu.make_async_copy(a, b, sems.at[n]) for n, (a, b) in enumerate(moves)]
    for copy in copies:
        copy.start()
    copies[0].wait()
    onehots = []
    for flip in flips:
        row = slots[pl.ds(jnp.bitwise_xor(seq_at, flip), 1), :]
        local = jnp.clip(own_slot_column(row, seq_at, cap) - seq_at * block, 0, block - 1)
        onehots.append((iota((cap, block), 1) == local).astype(F32).astype(BF16))
    first = 2 * block
    for copy, held in zip(copies[1:3], (q_in, r_in)):
        copy.wait()
        for out, flip, onehot in zip(outs, flips, onehots):
            source = held[jnp.bitwise_xor(seq_at, flip)]
            picked = jnp.dot(onehot, source, preferred_element_type=F32).astype(BF16)
            for h in range(picked.shape[1] // HD):
                out[first + h * cap : first + (h + 1) * cap, :] = picked[:, h * HD : (h + 1) * HD]
        first += q_in.shape[2] // HD * cap
    for copy in copies[3:]:
        copy.wait()


def completion_kernel(flips, block, slots, weight, *refs):
    parcels, (out, attended) = refs[: len(flips)], refs[len(flips) :]
    width = weight.shape[1]
    heads = weight.shape[0] // HD
    seq_at = lax.axis_index("seq")
    cap = attended.shape[0] // len(flips)
    row = slots[pl.ds(seq_at, 1), :]
    owners = [jnp.bitwise_xor(seq_at, flip) for flip in flips]
    span = block * len(flips)
    lane = iota((1, span), 1)
    key_pos = jnp.zeros((1, span), jnp.int32)
    reach = []
    for n, owner in enumerate(owners):
        key_pos = jnp.where(lane // block == n, lane + (owner - n) * block, key_pos)
        reach += [jnp.maximum(own_slot_column(row, owner, cap), 0)] * heads
    first = 2 * block
    last = first + heads * cap
    keys = jnp.concatenate([p[:block, :] for p in parcels], axis=0)
    values = jnp.concatenate([p[block:first, :] for p in parcels], axis=0)
    query = jnp.concatenate([p[first:last, :] for p in parcels], axis=0)
    scores = lax.dot_general(
        query, keys, (((1,), (1,)), ((), ())), preferred_element_type=F32
    ) * HD ** (-0.5)
    allowed = key_pos <= jnp.concatenate(reach, axis=0)
    scores = jnp.where(allowed, scores, FLOOR)
    top = jnp.max(scores, axis=1, keepdims=True)
    weights = jnp.where(allowed, jnp.exp(scores - top), 0.0)
    total = jnp.sum(weights, axis=1, keepdims=True)
    mixed = jnp.dot(weights.astype(BF16), values, preferred_element_type=F32)
    mixed = (mixed / total).astype(BF16)
    for n, (owner, parcel) in enumerate(zip(owners, parcels)):
        spot = pl.ds(pl.multiple_of(owner * cap, cap), cap)
        begin = n * heads * cap
        attended[spot, :] = jnp.concatenate(
            [mixed[begin + h * cap : begin + (h + 1) * cap, :] for h in range(heads)], axis=1
        )
        count = (out.shape[1] - width) // HD
        out[spot, width:] = jnp.concatenate(
            [parcel[last + h * cap : last + (h + 1) * cap, :] for h in range(count)], axis=1
        )
    total = jnp.dot(attended[...], weight[...], preferred_element_type=F32)
    out[:, :width] = total.astype(BF16)


def pair_norm_kernel(mine, other, gain, full, half):
    width = gain.shape[1]
    low = jnp.concatenate([mine[:, width:], other[:, width:]], axis=1)
    high = jnp.concatenate([other[:, width:], mine[:, width:]], axis=1)
    residual = jnp.where(lax.axis_index("vocab") == 0, low, high)
    norm_kernel(mine[:, :width], other[:, :width], residual, gain, full, half)


def norm_kernel(mine, other, residual, gain, full, half):
    hidden = residual[...].astype(F32) + (mine[...].astype(F32) + other[...].astype(F32))
    power = jnp.mean(hidden * hidden, axis=-1, keepdims=True)
    full[...] = (hidden * lax.rsqrt(power + 1e-06) * gain[...]).astype(BF16)
    if half is not None:
        count = half.shape[0]
        start = pl.multiple_of(lax.axis_index("vocab") * count, count)
        half[...] = full[pl.ds(start, count), :]


def fold(logits, wanted, first_row, top_ref, sum_ref, pick_ref):
    count, width = logits.shape
    tiles = logits.reshape(count // 8, 8, width)
    old = top_ref[...]
    new = jnp.maximum(old, jnp.max(tiles, axis=0))
    grown = jnp.sum(jnp.exp(tiles - new[None]), axis=0)
    sum_ref[...] = sum_ref[...] * jnp.exp(old - new) + grown
    top_ref[...] = new
    rows = iota(tiles.shape, 0) * 8 + iota(tiles.shape, 1)
    hit = rows == (wanted - first_row)[None]
    pick_ref[...] += jnp.sum(jnp.where(hit, tiles, 0.0), axis=0)


def score_tile(head, states, wanted, buffers, top_ref, sum_ref, pick_ref, step, unroll, base):
    top_ref[...] = jnp.full(top_ref.shape, FLOOR, F32)
    sum_ref[...] = jnp.zeros(sum_ref.shape, F32)
    pick_ref[...] = jnp.zeros(pick_ref.shape, F32)
    buffers[1][...] = jnp.full(buffers[1].shape, FLOOR, F32)
    local = wanted - base
    local = jnp.where((local >= 0) & (local < head.shape[0]), local, -(1 << 30))
    local = jnp.broadcast_to(local, top_ref.shape)

    def body(at, carry):
        for j in range(unroll):
            first = at * (unroll * step) + j * step
            block = head[pl.ds(pl.multiple_of(first, step), step), :]
            logits = lax.dot_general(
                block, states[...], (((1,), (1,)), ((), ())), preferred_element_type=F32
            )
            fold(buffers[(j + 1) % 2][...], local, first - step, top_ref, sum_ref, pick_ref)
            buffers[j % 2][...] = logits
        return carry

    total = head.shape[0]
    lax.fori_loop(0, total // (unroll * step), body, 0)
    fold(buffers[(unroll - 1) % 2][...], local, total - step, top_ref, sum_ref, pick_ref)
    top = jnp.max(top_ref[...], axis=0, keepdims=True)
    scale = jnp.exp(top_ref[...] - top)
    total = jnp.sum(sum_ref[...] * scale, axis=0, keepdims=True)
    return top + jnp.log(total), jnp.sum(pick_ref[...], axis=0, keepdims=True)


def vocab_base(shard_rows):
    owner = lax.axis_index("seq") * lax.axis_size("sample") + lax.axis_index("sample")
    return (owner * lax.axis_size("vocab") + lax.axis_index("vocab")) * shard_rows


def steps_of(shard_rows):
    for step in (256, 128, 64, 32, 16, 8):
        if shard_rows % (2 * step) == 0:
            unroll = next(n for n in (20, 10, 4, 2) if shard_rows % (n * step) == 0)
            return step, unroll
    raise ValueError("head rows")


def column_kernel(places, step, unroll, last, head, meta, other_meta, *refs):
    before, refs = (refs[0], refs[1:]) if last is not None else (None, refs)
    count = sum(abs(place[2]) for place in places)
    inputs, refs = refs[:count], refs[count:]
    out, states, buf_a, buf_b, top_ref, sum_ref, pick_ref = refs[:7]
    rows = meta.shape[1]
    seq_at, core = lax.axis_index("seq"), lax.axis_index("vocab")
    wanted = []
    for n, place in enumerate(places):
        held = inputs[: abs(place[2])]
        inputs = inputs[abs(place[2]) :]
        if place[2] < 0:
            for part, ref in enumerate(held):

                @pl.when(core == 1 - part)
                def _(ref=ref, n=n):
                    states[n * rows : (n + 1) * rows, :] = ref[...]
        else:
            for part, ref in enumerate(held):
                count = ref.shape[0]
                start = n * rows
                if len(held) > 1:
                    start = pl.multiple_of(start + jnp.bitwise_xor(core, part) * count, count)
                states[pl.ds(start, count), :] = ref[...]
        row = pl.ds(chip_of(place[1], seq_at, core), 1)
        column = of_core(place[0], core)
        wanted.append(jnp.where(column == 1, other_meta[row, :], meta[row, :]))
    logs, picks = score_tile(
        head, states, jnp.concatenate(wanted, axis=1), (buf_a, buf_b), top_ref, sum_ref, pick_ref,
        step, unroll, vocab_base(head.shape[0]),
    )
    results = [
        jnp.concatenate([logs[:, n * rows : (n + 1) * rows], picks[:, n * rows : (n + 1) * rows]], axis=1)
        for n in range(len(places))
    ]
    if last is None:
        for n, result in enumerate(results):
            out[n : n + 1, :] = result
        return
    message = refs[7]
    results = [before[n : n + 1, :] for n in range(len(last))] + results
    for place, result in zip([*last, *places], results):
        column = jnp.bitwise_xor(lax.axis_index("sample"), of_core(place[0], core))
        row = column * lax.axis_size("seq") + chip_of(place[1], seq_at, core)
        message[pl.ds(row, 1), :] = result
    out[...] = jnp.broadcast_to(message[...][None], out.shape)


def of_core(choice, core):
    return jnp.where(core == 0, *choice) if isinstance(choice, tuple) else choice


def chip_of(flip, seq_at, core):
    return jnp.bitwise_xor(seq_at, of_core(flip, core))


def column_scores(head, meta, other_meta, places, blocks, last=None, before=None):
    step, unroll = steps_of(head.shape[0])
    rows = meta.shape[1]
    total = rows * len(places)
    peers = 1
    for axis in CELL:
        peers *= lax.axis_size(axis)
    chips = peers // lax.axis_size("vocab")
    shape = (len(places), 2 * rows) if last is None else (peers, chips, 2 * rows)
    extra = [] if last is None else [before]
    return call(
        functools.partial(column_kernel, places, step, unroll, last),
        jax.ShapeDtypeStruct(shape, F32),
        [head, meta, other_meta, *extra, *blocks],
        [vmem()] * (3 + len(extra) + len(blocks)),
        scratch=[pltpu.VMEM((total, head.shape[1]), BF16)]
        + [pltpu.VMEM((step, total), F32)] * 2
        + [pltpu.VMEM((8, total), F32)] * 3
        + [pltpu.VMEM((chips, 2 * rows), F32)],
        flops=2 * total * head.shape[0] * head.shape[1],
    )


def tile_kernel(step, unroll, head, states, wanted, out, buf_a, buf_b, top_ref, sum_ref, pick_ref):
    parts = score_tile(
        head, states, wanted[...], (buf_a, buf_b), top_ref, sum_ref, pick_ref,
        step, unroll, vocab_base(head.shape[0]),
    )
    out[...] = jnp.concatenate(parts, axis=0)


def tiled_scores(head, states, wanted):
    step, unroll = steps_of(head.shape[0])
    count, width = states.shape
    tile = next(n for n in (256, 128, count) if count % n == 0)
    return pl.pallas_call(
        functools.partial(tile_kernel, step, unroll),
        grid=(count // tile,),
        out_shape=jax.ShapeDtypeStruct((2, count), F32),
        in_specs=[
            pl.BlockSpec(head.shape, lambda i: (0, 0)),
            pl.BlockSpec((tile, width), lambda i: (i, 0)),
            pl.BlockSpec((1, tile), lambda i: (0, i)),
        ],
        out_specs=pl.BlockSpec((2, tile), lambda i: (0, i)),
        scratch_shapes=[pltpu.VMEM((step, tile), F32)] * 2 + [pltpu.VMEM((8, tile), F32)] * 3,
        compiler_params=pltpu.CompilerParams(
            dimension_semantics=("arbitrary",), vmem_limit_bytes=52 * 2**20
        ),
    )(head, states, wanted)


def close_kernel(relative, columns, length, stats, *refs):
    metas, (tokens_out, scores_out, advantages_out, objective_out, tokens) = refs[:-5], refs[-5:]
    samples, cap = tokens_out.shape
    slots = tokens.shape[1]
    prompts = samples * columns
    where, seq_at = lax.axis_index("sample"), lax.axis_index("seq")
    metas = [ref[...] for ref in metas]
    if relative:
        metas = [jnp.where(where == k, metas[0], metas[1]) for k in range(columns)]
    top = stats[0]
    for s in range(1, stats.shape[0]):
        top = jnp.maximum(top, stats[s])
    total = jnp.exp(stats[0] - top)
    pick = stats[0]
    for s in range(1, stats.shape[0]):
        total += jnp.exp(stats[s] - top)
        pick += stats[s]
    logprob = pick[:, slots:] - (top + jnp.log(total))[:, :slots]
    wanted = jnp.concatenate([meta[:samples] for meta in metas], axis=0)
    tokens[...] = jnp.where(wanted >= 0, logprob, 0.0)
    paid = [meta[samples : samples + 1, :].astype(F32) for meta in metas]
    reward_sum = functools.reduce(lambda a, b: a + b, [jnp.sum(row) for row in paid])
    lane = iota((1, slots), 1)
    objective = jnp.float32(0)
    for k in range(columns):
        for i in range(samples):
            at = k * samples + i
            score = jnp.sum(tokens[at : at + 1, :]) / length
            reward = jnp.sum(jnp.where(lane == i, paid[k], 0.0))
            advantage = reward - (reward_sum - reward) / (prompts - 1)
            objective += advantage * score

            @pl.when(where == k)
            def _(score=score, advantage=advantage, i=i):
                scores_out[i] = score
                advantages_out[i] = advantage

    objective_out[0] = -(objective / prompts)
    mine = tokens[:samples, :]
    for k in range(1, columns):
        mine = jnp.where(where == k, tokens[k * samples : (k + 1) * samples, :], mine)
    piece = mine[:, :cap]
    for n in range(1, slots // cap):
        piece = jnp.where(seq_at == n, mine[:, n * cap : (n + 1) * cap], piece)
    tokens_out[...] = piece


def close(stats, metas, relative, samples, cap, length):
    columns = lax.axis_size("sample")
    outs = (
        jax.ShapeDtypeStruct((samples, cap), F32),
        jax.ShapeDtypeStruct((samples,), F32),
        jax.ShapeDtypeStruct((samples,), F32),
        jax.ShapeDtypeStruct((1,), F32),
    )
    return call(
        functools.partial(close_kernel, relative, columns, length),
        outs,
        [stats, *metas],
        [vmem()] * (1 + len(metas)),
        out_specs=(vmem(), smem(), smem(), smem()),
        scratch=[pltpu.VMEM((stats.shape[1], stats.shape[2] // 2), F32)],
    )


def steps(
    queries, key_states, value_states, residual, out_weight, norm_gain,
    vocab_head, targets, scored_slots, lengths, rewards,
):
    samples, block, width = queries.shape
    model_width = out_weight.shape[1]
    seq_size, sample_size, vocab_size = (lax.axis_size(axis) for axis in CELL)
    cap = scored_slots.shape[1] // seq_size
    length = targets.shape[1]
    rows = samples * cap
    sizes = tuple(lax.axis_size(axis) for axis in ("groups",) + CELL)
    short = sizes == (2, 4, 2, 2) and samples == seq_size and key_states.shape[2] == HD

    def send(array, target):
        pairs = []
        for z in range(seq_size):
            for x in range(sample_size):
                for c in range(vocab_size):
                    place = target(z, x, c)
                    if place is not None:
                        source = (z * sample_size + x) * vocab_size + c
                        to = (place[0] * sample_size + place[1]) * vocab_size + place[2]
                        pairs.append((source, to))
        return lax.ppermute(array, CELL, pairs)

    def aside(array):
        pairs = []
        for g in range(2):
            for z in range(seq_size):
                for x in range(sample_size):
                    at = ((g * seq_size + z) * sample_size + x) * vocab_size
                    pairs.append((at, (((1 - g) * seq_size + z) * sample_size + x) * vocab_size))
                    pairs.append((at + 1, ((g * seq_size + z) * sample_size + 1 - x) * vocab_size + 1))
        return lax.ppermute(array, ("groups",) + CELL, pairs)

    def across(array):
        return send(array, lambda z, x, c: (z, x, c ^ 1))

    def beside(array):
        return send(array, lambda z, x, c: (z, x ^ 1, c))

    flips = (0, 2, 3, 1)
    if short:
        half_width = model_width // vocab_size
        parcel_rows = 2 * block + (width + half_width) // HD * cap
        parcels = call(
            functools.partial(parcel_kernel, flips),
            tuple(jax.ShapeDtypeStruct((parcel_rows, HD), BF16) for _ in flips),
            [keep(a) for a in (scored_slots, key_states, value_states, queries, residual)],
            [hbm()] * 5,
            scratch=[
                pltpu.VMEM(scored_slots.shape, jnp.int32),
                pltpu.VMEM(queries.shape, BF16),
                pltpu.VMEM((samples, block, half_width), BF16),
                pltpu.SemaphoreType.DMA((3 + 2 * len(flips),)),
            ],
        )
        far = send(parcels[1], lambda z, x, c: (z ^ 2, x, c))
        wrap = send(parcels[2], lambda z, x, c: (z ^ 3, x, c))
        near = send(parcels[3], lambda z, x, c: (z ^ 1, x, c))
        blocks = [parcels[0], far, wrap, near]
    else:
        offsets = (0,)
        kv_shape = (samples, block, 2 * key_states.shape[2])
        pair = call(
            pack_kernel,
            jax.ShapeDtypeStruct(kv_shape, BF16),
            [keep(key_states), keep(value_states)],
            [hbm(), hbm()],
            scratch=[pltpu.SemaphoreType.DMA((2,))],
            limit=4,
        )
        blocks = [lax.all_gather(pair, "seq", axis=1, tiled=True)]
    heads = width // HD
    slots, picked, picked_resid, meta, weight, gain = call(
        prep_kernel,
        (
            jax.ShapeDtypeStruct(scored_slots.shape, jnp.int32),
            jax.ShapeDtypeStruct((samples, heads * cap, HD), BF16),
            jax.ShapeDtypeStruct((rows, model_width), BF16),
            jax.ShapeDtypeStruct((samples + 1, scored_slots.shape[1]), jnp.int32),
            pltpu.VMEM(out_weight.shape, BF16),
            pltpu.VMEM((1, model_width), F32),
        ),
        [
            keep(array)
            for array in (
                scored_slots, targets, lengths, rewards, queries, residual,
                out_weight, norm_gain,
            )
        ],
        [hbm()] * 8,
        scratch=[
            pltpu.VMEM(targets.shape, jnp.int32),
            pltpu.SMEM(lengths.shape, jnp.int32),
            pltpu.SMEM(rewards.shape, jnp.int32),
            pltpu.VMEM(queries.shape, BF16),
            pltpu.VMEM(residual.shape, BF16),
            pltpu.SemaphoreType.DMA((8,)),
        ],
        limit=12,
    )
    head = pltpu.with_memory_space_constraint(vocab_head, pltpu.VMEM)
    weight = pltpu.with_memory_space_constraint(weight, pltpu.VMEM)
    if short:
        partial_value = call(
            functools.partial(completion_kernel, flips, block),
            jax.ShapeDtypeStruct((rows, model_width + half_width), BF16),
            [slots, weight, *blocks],
            [vmem()] * (2 + len(blocks)),
            scratch=[pltpu.VMEM((rows, width), BF16)],
            flops=10**10,
        )
    else:
        partial_value = call(
            functools.partial(attend_kernel, offsets),
            jax.ShapeDtypeStruct((rows, model_width), BF16),
            [slots, picked, weight, *blocks],
            [vmem()] * (3 + len(blocks)),
        )
    if short:
        other_meta = beside(meta)
        other_partial = across(partial_value)
        normed, half = call(
            pair_norm_kernel,
            (
                jax.ShapeDtypeStruct((rows, model_width), BF16),
                jax.ShapeDtypeStruct((rows // 2, model_width), BF16),
            ),
            [partial_value, other_partial, gain],
            [vmem()] * 3,
        )
        split = send(normed, lambda z, x, c: (z ^ (1, 3)[c], x, c))
        side = beside(half)
        turn = send(split, lambda z, x, c: (z, x ^ 1, c) if c == 0 else (z ^ 1, x, c))
        split_side = aside(split)
        side_far = send(side, lambda z, x, c: (z ^ 2, x, c))
        split_other = across(split)
        side_other = across(side)
        turn_other = across(turn)
        split_side_other = across(split_side)
        side_far_other = across(side_far)
        near = [(0, 0, 1), (0, (1, 3), 1), (0, (3, 1), 1), (1, 0, 2)]
        rest = [((1, 0), (1, 2), 1), ((0, 1), (2, 1), 1), (1, 3, -2), (1, 2, 2)]
        first = column_scores(
            head, meta, other_meta, near, [normed, split, split_other, side, side_other]
        )
        stats = column_scores(
            head, meta, other_meta, rest,
            [turn, turn_other, split_side, split_side_other, side_far, side_far_other],
            last=near, before=first,
        )
        stats = lax.all_to_all(stats, CELL, 0, 0, tiled=True)
        return close(stats, [meta, other_meta], True, samples, cap, length)
    summed = lax.psum(partial_value, "vocab")
    normed = call(
        lambda a, b, r, g, out: norm_kernel(a, b, r, g, out, None),
        jax.ShapeDtypeStruct((rows, model_width), BF16),
        [summed, jnp.zeros_like(summed), picked_resid, gain],
        [vmem()] * 4,
    )
    every = lax.all_gather(normed, "seq", axis=0, tiled=True)
    every = lax.all_gather(every, "sample", axis=0, tiled=True)
    metas = lax.all_gather(meta, "sample", axis=0)
    by_chip = (sample_size, samples, seq_size, cap)
    wanted = metas[:, :samples].reshape(by_chip).transpose(0, 2, 1, 3).reshape(1, -1)
    logs, picks = tiled_scores(vocab_head, every, wanted)
    top = lax.pmax(logs, CELL)
    total, pick = lax.psum((jnp.exp(logs - top), picks), CELL)
    by_row = (sample_size, seq_size, samples, cap)
    stats = [
        part.reshape(by_row).transpose(0, 2, 1, 3).reshape(1, sample_size * samples, seq_size * cap)
        for part in (top + jnp.log(total), pick)
    ]
    stats = jnp.concatenate(stats, axis=2)
    metas = [metas[k] for k in range(sample_size)]
    return close(stats, metas, False, samples, cap, length)


def solution(mesh):
    in_specs = (
        P(("groups", "sample"), "seq", "vocab"),
        P(("groups", "sample"), "seq", "vocab"),
        P(("groups", "sample"), "seq", "vocab"),
        P(("groups", "sample"), "seq", None),
        P("vocab", None),
        P(),
        P(("seq", "sample", "vocab"), None),
        P(("groups", "sample"), None),
        P(("groups", "sample"), None),
        P(("groups", "sample")),
        P(("groups", "sample")),
    )
    out_specs = (
        P(("groups", "sample"), "seq"),
        P(("groups", "sample")),
        P(("groups", "sample")),
        P("groups"),
    )
    step = jax.shard_map(steps, mesh=mesh, in_specs=in_specs, out_specs=out_specs, check_vma=False)
    if tuple(mesh.shape[axis] for axis in ("groups",) + CELL) != (2, 4, 2, 2):
        return step
    return step
```

```python
import functools

import jax
import jax.numpy as jnp
from jax import lax
from jax.experimental import pallas as pl
from jax.experimental.pallas import tpu as pltpu
from jax.sharding import PartitionSpec as P


HD = 128
F32 = jnp.float32
BF16 = jnp.bfloat16
FLOOR = -1e30
CELL = ("seq", "sample", "vocab")


def vmem():
    return pl.BlockSpec(memory_space=pltpu.VMEM)


def hbm():
    return pl.BlockSpec(memory_space=pltpu.HBM)


def keep(array):
    return pltpu.with_memory_space_constraint(array, pltpu.HBM)


def smem():
    return pl.BlockSpec(memory_space=pltpu.SMEM)


def call(body, outs, ins, in_specs, out_specs=None, scratch=(), limit=12, flops=None):
    cost = None
    if flops is not None:
        cost = pl.CostEstimate(flops=flops, bytes_accessed=0, transcendentals=0)
    return pl.pallas_call(
        body,
        cost_estimate=cost,
        out_shape=outs,
        in_specs=in_specs,
        out_specs=jax.tree.map(lambda _: vmem(), outs) if out_specs is None else out_specs,
        scratch_shapes=list(scratch),
        compiler_params=pltpu.CompilerParams(vmem_limit_bytes=limit * 2**20),
    )(*ins)


def iota(shape, dim):
    return lax.broadcasted_iota(jnp.int32, shape, dim)


def own_slot_column(slots_row, seq_at, cap):
    total = slots_row.shape[1]
    hit = iota((cap, total), 1) == iota((cap, total), 0) + seq_at * cap
    return jnp.sum(jnp.where(hit, slots_row, 0), axis=1, keepdims=True)


def pack_kernel(keys, values, out, sems):
    width = keys.shape[2]
    copies = [
        pltpu.make_async_copy(ref, out.at[:, :, pl.ds(n * width, width)], sems.at[n])
        for n, ref in enumerate((keys, values))
    ]
    for copy in copies:
        copy.start()
    for copy in copies:
        copy.wait()


def prep_kernel(
    slots_in, targets_in, lengths_in, rewards_in, queries, residual, weight, gain,
    slots, q_out, r_out, meta_out, weight_out, gain_out,
    targets, lengths, rewards, q_in, r_in, sems,
):
    samples, block, width = queries.shape
    total, length = slots.shape[1], targets.shape[1]
    heads = width // HD
    cap = r_out.shape[0] // samples
    seq_at = lax.axis_index("seq")
    lanes = meta_out.shape[1]
    moves = [
        (slots_in, slots), (targets_in, targets), (lengths_in, lengths), (rewards_in, rewards),
        (queries, q_in), (residual, r_in), (weight, weight_out), (gain, gain_out.at[0]),
    ]
    copies = [pltpu.make_async_copy(a, b, sems.at[n]) for n, (a, b) in enumerate(moves)]
    for copy in copies:
        copy.start()
    for copy in copies[:4]:
        copy.wait()
    reward_row = jnp.zeros((1, lanes), jnp.int32)
    onehots = []
    for i in range(samples):
        row = slots[i : i + 1, :]
        local = jnp.clip(own_slot_column(row, seq_at, cap) - seq_at * block, 0, block - 1)
        onehots.append((iota((cap, block), 1) == local).astype(F32).astype(BF16))
        eye = iota((total, total), 0) == iota((total, total), 1)
        column = jnp.sum(jnp.where(eye, jnp.maximum(row, 0), 0), axis=1, keepdims=True)
        spot = iota((total, length), 1) == column
        found = jnp.sum(jnp.where(spot, targets[i : i + 1, :], 0), axis=1, keepdims=True)
        wanted = jnp.sum(jnp.where(eye, found, 0), axis=0, keepdims=True)
        meta_out[i : i + 1, :] = jnp.where((row >= 0) & (row < lengths[i]), wanted, -1)
        reward_row = jnp.where(iota((1, lanes), 1) == i, rewards[i], reward_row)
    meta_out[samples : samples + 1, :] = reward_row
    copies[4].wait()
    for i in range(samples):
        picked = jnp.dot(onehots[i], q_in[i], preferred_element_type=F32).astype(BF16)
        for h in range(heads):
            q_out[i, h * cap : (h + 1) * cap, :] = picked[:, h * HD : (h + 1) * HD]
    copies[5].wait()
    for i in range(samples):
        r_out[i * cap : (i + 1) * cap, :] = jnp.dot(
            onehots[i], r_in[i], preferred_element_type=F32
        ).astype(BF16)
    for copy in copies[6:]:
        copy.wait()


def attend_kernel(offsets, slots, queries, weight, *refs):
    blocks, out = refs[:-1], refs[-1]
    samples, stacked, _ = queries.shape
    block_len, kv_width = blocks[0].shape[1], blocks[0].shape[2]
    kv_heads = kv_width // (2 * HD)
    heads = weight.shape[0] // HD
    cap = stacked // heads
    group = heads // kv_heads
    span = block_len * len(blocks)
    seq_at = lax.axis_index("seq")
    lane = iota((1, span), 1)
    key_pos = lane
    if len(blocks) > 1:
        key_pos = jnp.zeros((1, span), jnp.int32)
        for n, flip in enumerate(offsets):
            start = jnp.bitwise_xor(seq_at, flip) * block_len
            key_pos = jnp.where(lane // block_len == n, lane - n * block_len + start, key_pos)
    rows = []
    for i in range(samples):
        column = jnp.maximum(own_slot_column(slots[i : i + 1, :], seq_at, cap), 0)
        reach = jnp.concatenate([column] * group, axis=0)
        allowed = key_pos <= reach
        pieces = []
        for g in range(kv_heads):
            left, right = g * HD, kv_width // 2 + g * HD
            keys = jnp.concatenate([b[i, :, left : left + HD] for b in blocks], axis=0)
            values = jnp.concatenate([b[i, :, right : right + HD] for b in blocks], axis=0)
            query = queries[i, g * group * cap : (g + 1) * group * cap, :]
            scores = lax.dot_general(
                query, keys, (((1,), (1,)), ((), ())), preferred_element_type=F32
            ) * HD ** (-0.5)
            scores = jnp.where(allowed, scores, FLOOR)
            top = jnp.max(scores, axis=1, keepdims=True)
            weights = jnp.where(allowed, jnp.exp(scores - top), 0.0)
            total = jnp.sum(weights, axis=1, keepdims=True)
            mixed = jnp.dot(weights.astype(BF16), values, preferred_element_type=F32)
            mixed = (mixed / total).astype(BF16)
            pieces += [mixed[h * cap : (h + 1) * cap, :] for h in range(group)]
        rows.append(jnp.concatenate(pieces, axis=1))
    attended = jnp.concatenate(rows, axis=0)
    out[...] = jnp.dot(attended, weight[...], preferred_element_type=F32).astype(BF16)


def parcel_kernel(flips, slots_in, keys, values, queries, residual, *refs):
    outs, (slots, q_in, r_in, sems) = refs[: len(flips)], refs[len(flips) :]
    samples, block, _ = queries.shape
    half = r_in.shape[2]
    seq_at = lax.axis_index("seq")
    cap = slots.shape[1] // samples
    start = pl.multiple_of(lax.axis_index("vocab") * half, half)
    takers = [jnp.bitwise_xor(seq_at, flip) for flip in flips]
    moves = [(slots_in, slots)]
    moves += [(queries.at[taker], q_in.at[n]) for n, taker in enumerate(takers)]
    moves += [(residual.at[taker, :, pl.ds(start, half)], r_in.at[n]) for n, taker in enumerate(takers)]
    for out, taker in zip(outs, takers):
        moves.append((keys.at[taker], out.at[pl.ds(0, block), :]))
        moves.append((values.at[taker], out.at[pl.ds(block, block), :]))
    copies = [pltpu.make_async_copy(a, b, sems.at[n]) for n, (a, b) in enumerate(moves)]
    for copy in copies:
        copy.start()
    copies[0].wait()
    onehots = []
    for flip in flips:
        row = slots[pl.ds(jnp.bitwise_xor(seq_at, flip), 1), :]
        local = jnp.clip(own_slot_column(row, seq_at, cap) - seq_at * block, 0, block - 1)
        onehots.append((iota((cap, block), 1) == local).astype(F32).astype(BF16))
    first, at = 2 * block, 1
    for held in (q_in, r_in):
        for n, (out, onehot) in enumerate(zip(outs, onehots)):
            copies[at].wait()
            at += 1
            picked = jnp.dot(onehot, held[n], preferred_element_type=F32).astype(BF16)
            for h in range(picked.shape[1] // HD):
                out[first + h * cap : first + (h + 1) * cap, :] = picked[:, h * HD : (h + 1) * HD]
        first += q_in.shape[2] // HD * cap
    for copy in copies[at:]:
        copy.wait()


def completion_kernel(flips, block, slots, weight, *refs):
    parcels, (out, attended) = refs[: len(flips)], refs[len(flips) :]
    width = weight.shape[1]
    heads = weight.shape[0] // HD
    seq_at = lax.axis_index("seq")
    cap = attended.shape[0] // len(flips)
    row = slots[pl.ds(seq_at, 1), :]
    owners = [jnp.bitwise_xor(seq_at, flip) for flip in flips]
    span = block * len(flips)
    lane = iota((1, span), 1)
    key_pos = jnp.zeros((1, span), jnp.int32)
    reach = []
    for n, owner in enumerate(owners):
        key_pos = jnp.where(lane // block == n, lane + (owner - n) * block, key_pos)
        reach += [jnp.maximum(own_slot_column(row, owner, cap), 0)] * heads
    first = 2 * block
    last = first + heads * cap
    keys = jnp.concatenate([p[:block, :] for p in parcels], axis=0)
    values = jnp.concatenate([p[block:first, :] for p in parcels], axis=0)
    query = jnp.concatenate([p[first:last, :] for p in parcels], axis=0)
    scores = lax.dot_general(
        query, keys, (((1,), (1,)), ((), ())), preferred_element_type=F32
    ) * HD ** (-0.5)
    allowed = key_pos <= jnp.concatenate(reach, axis=0)
    scores = jnp.where(allowed, scores, FLOOR)
    top = jnp.max(scores, axis=1, keepdims=True)
    weights = jnp.where(allowed, jnp.exp(scores - top), 0.0)
    total = jnp.sum(weights, axis=1, keepdims=True)
    mixed = jnp.dot(weights.astype(BF16), values, preferred_element_type=F32)
    mixed = (mixed / total).astype(BF16)
    for n, (owner, parcel) in enumerate(zip(owners, parcels)):
        spot = pl.ds(pl.multiple_of(owner * cap, cap), cap)
        begin = n * heads * cap
        attended[spot, :] = jnp.concatenate(
            [mixed[begin + h * cap : begin + (h + 1) * cap, :] for h in range(heads)], axis=1
        )
        count = (out.shape[1] - width) // HD
        out[spot, width:] = jnp.concatenate(
            [parcel[last + h * cap : last + (h + 1) * cap, :] for h in range(count)], axis=1
        )
    total = jnp.dot(attended[...], weight[...], preferred_element_type=F32)
    out[:, :width] = total.astype(BF16)


def pair_norm_kernel(mine, other, gain, full, half):
    width = gain.shape[1]
    low = jnp.concatenate([mine[:, width:], other[:, width:]], axis=1)
    high = jnp.concatenate([other[:, width:], mine[:, width:]], axis=1)
    residual = jnp.where(lax.axis_index("vocab") == 0, low, high)
    norm_kernel(mine[:, :width], other[:, :width], residual, gain, full, half)


def norm_kernel(mine, other, residual, gain, full, half):
    hidden = residual[...].astype(F32) + (mine[...].astype(F32) + other[...].astype(F32))
    power = jnp.mean(hidden * hidden, axis=-1, keepdims=True)
    full[...] = (hidden * lax.rsqrt(power + 1e-06) * gain[...]).astype(BF16)
    if half is not None:
        count = half.shape[0]
        start = pl.multiple_of(lax.axis_index("vocab") * count, count)
        half[...] = full[pl.ds(start, count), :]


def fold(logits, wanted, first_row, top_ref, sum_ref, pick_ref):
    count, width = logits.shape
    tiles = logits.reshape(count // 8, 8, width)
    old = top_ref[...]
    new = jnp.maximum(old, jnp.max(tiles, axis=0))
    grown = jnp.sum(jnp.exp(tiles - new[None]), axis=0)
    sum_ref[...] = sum_ref[...] * jnp.exp(old - new) + grown
    top_ref[...] = new
    rows = iota(tiles.shape, 0) * 8 + iota(tiles.shape, 1)
    hit = rows == (wanted - first_row)[None]
    pick_ref[...] += jnp.sum(jnp.where(hit, tiles, 0.0), axis=0)


def score_tile(head, states, wanted, buffers, top_ref, sum_ref, pick_ref, step, unroll, base):
    top_ref[...] = jnp.full(top_ref.shape, FLOOR, F32)
    sum_ref[...] = jnp.zeros(sum_ref.shape, F32)
    pick_ref[...] = jnp.zeros(pick_ref.shape, F32)
    buffers[1][...] = jnp.full(buffers[1].shape, FLOOR, F32)
    local = wanted - base
    local = jnp.where((local >= 0) & (local < head.shape[0]), local, -(1 << 30))
    local = jnp.broadcast_to(local, top_ref.shape)

    def body(at, carry):
        for j in range(unroll):
            first = at * (unroll * step) + j * step
            block = head[pl.ds(pl.multiple_of(first, step), step), :]
            logits = lax.dot_general(
                block, states[...], (((1,), (1,)), ((), ())), preferred_element_type=F32
            )
            fold(buffers[(j + 1) % 2][...], local, first - step, top_ref, sum_ref, pick_ref)
            buffers[j % 2][...] = logits
        return carry

    total = head.shape[0]
    lax.fori_loop(0, total // (unroll * step), body, 0)
    fold(buffers[(unroll - 1) % 2][...], local, total - step, top_ref, sum_ref, pick_ref)
    top = jnp.max(top_ref[...], axis=0, keepdims=True)
    scale = jnp.exp(top_ref[...] - top)
    total = jnp.sum(sum_ref[...] * scale, axis=0, keepdims=True)
    return top + jnp.log(total), jnp.sum(pick_ref[...], axis=0, keepdims=True)


def vocab_base(shard_rows):
    owner = lax.axis_index("seq") * lax.axis_size("sample") + lax.axis_index("sample")
    return (owner * lax.axis_size("vocab") + lax.axis_index("vocab")) * shard_rows


def steps_of(shard_rows):
    for step in (256, 128, 64, 32, 16, 8):
        if shard_rows % (2 * step) == 0:
            unroll = next(n for n in (20, 10, 4, 2) if shard_rows % (n * step) == 0)
            return step, unroll
    raise ValueError("head rows")


def column_kernel(places, step, unroll, last, head, meta, other_meta, *refs):
    before, refs = (refs[0], refs[1:]) if last is not None else (None, refs)
    count = sum(abs(place[2]) for place in places)
    inputs, refs = refs[:count], refs[count:]
    out, states, buf_a, buf_b, top_ref, sum_ref, pick_ref = refs[:7]
    rows = meta.shape[1]
    seq_at, core = lax.axis_index("seq"), lax.axis_index("vocab")
    wanted = []
    for n, place in enumerate(places):
        held = inputs[: abs(place[2])]
        inputs = inputs[abs(place[2]) :]
        if place[2] < 0:
            for part, ref in enumerate(held):

                @pl.when(core == 1 - part)
                def _(ref=ref, n=n):
                    states[n * rows : (n + 1) * rows, :] = ref[...]
        else:
            for part, ref in enumerate(held):
                count = ref.shape[0]
                start = n * rows
                if len(held) > 1:
                    start = pl.multiple_of(start + jnp.bitwise_xor(core, part) * count, count)
                states[pl.ds(start, count), :] = ref[...]
        row = pl.ds(chip_of(place[1], seq_at, core), 1)
        column = of_core(place[0], core)
        wanted.append(jnp.where(column == 1, other_meta[row, :], meta[row, :]))
    logs, picks = score_tile(
        head, states, jnp.concatenate(wanted, axis=1), (buf_a, buf_b), top_ref, sum_ref, pick_ref,
        step, unroll, vocab_base(head.shape[0]),
    )
    results = [
        jnp.concatenate([logs[:, n * rows : (n + 1) * rows], picks[:, n * rows : (n + 1) * rows]], axis=1)
        for n in range(len(places))
    ]
    if last is None:
        for n, result in enumerate(results):
            out[n : n + 1, :] = result
        return
    message = refs[7]
    results = [before[n : n + 1, :] for n in range(len(last))] + results
    for place, result in zip([*last, *places], results):
        column = jnp.bitwise_xor(lax.axis_index("sample"), of_core(place[0], core))
        row = column * lax.axis_size("seq") + chip_of(place[1], seq_at, core)
        message[pl.ds(row, 1), :] = result
    out[...] = jnp.broadcast_to(message[...][None], out.shape)


def of_core(choice, core):
    return jnp.where(core == 0, *choice) if isinstance(choice, tuple) else choice


def chip_of(flip, seq_at, core):
    return jnp.bitwise_xor(seq_at, of_core(flip, core))


def column_scores(head, meta, other_meta, places, blocks, last=None, before=None):
    step, unroll = steps_of(head.shape[0])
    rows = meta.shape[1]
    total = rows * len(places)
    peers = 1
    for axis in CELL:
        peers *= lax.axis_size(axis)
    chips = peers // lax.axis_size("vocab")
    shape = (len(places), 2 * rows) if last is None else (peers, chips, 2 * rows)
    extra = [] if last is None else [before]
    return call(
        functools.partial(column_kernel, places, step, unroll, last),
        jax.ShapeDtypeStruct(shape, F32),
        [head, meta, other_meta, *extra, *blocks],
        [vmem()] * (3 + len(extra) + len(blocks)),
        scratch=[pltpu.VMEM((total, head.shape[1]), BF16)]
        + [pltpu.VMEM((step, total), F32)] * 2
        + [pltpu.VMEM((8, total), F32)] * 3
        + [pltpu.VMEM((chips, 2 * rows), F32)],
        flops=2 * total * head.shape[0] * head.shape[1],
    )


def tile_kernel(step, unroll, head, states, wanted, out, buf_a, buf_b, top_ref, sum_ref, pick_ref):
    parts = score_tile(
        head, states, wanted[...], (buf_a, buf_b), top_ref, sum_ref, pick_ref,
        step, unroll, vocab_base(head.shape[0]),
    )
    out[...] = jnp.concatenate(parts, axis=0)


def tiled_scores(head, states, wanted):
    step, unroll = steps_of(head.shape[0])
    count, width = states.shape
    tile = next(n for n in (256, 128, count) if count % n == 0)
    return pl.pallas_call(
        functools.partial(tile_kernel, step, unroll),
        grid=(count // tile,),
        out_shape=jax.ShapeDtypeStruct((2, count), F32),
        in_specs=[
            pl.BlockSpec(head.shape, lambda i: (0, 0)),
            pl.BlockSpec((tile, width), lambda i: (i, 0)),
            pl.BlockSpec((1, tile), lambda i: (0, i)),
        ],
        out_specs=pl.BlockSpec((2, tile), lambda i: (0, i)),
        scratch_shapes=[pltpu.VMEM((step, tile), F32)] * 2 + [pltpu.VMEM((8, tile), F32)] * 3,
        compiler_params=pltpu.CompilerParams(
            dimension_semantics=("arbitrary",), vmem_limit_bytes=52 * 2**20
        ),
    )(head, states, wanted)


def close_kernel(relative, columns, length, stats, *refs):
    metas, (tokens_out, scores_out, advantages_out, objective_out, tokens) = refs[:-5], refs[-5:]
    samples, cap = tokens_out.shape
    slots = tokens.shape[1]
    prompts = samples * columns
    where, seq_at = lax.axis_index("sample"), lax.axis_index("seq")
    metas = [ref[...] for ref in metas]
    if relative:
        metas = [jnp.where(where == k, metas[0], metas[1]) for k in range(columns)]
    top = stats[0]
    for s in range(1, stats.shape[0]):
        top = jnp.maximum(top, stats[s])
    total = jnp.exp(stats[0] - top)
    pick = stats[0]
    for s in range(1, stats.shape[0]):
        total += jnp.exp(stats[s] - top)
        pick += stats[s]
    logprob = pick[:, slots:] - (top + jnp.log(total))[:, :slots]
    wanted = jnp.concatenate([meta[:samples] for meta in metas], axis=0)
    tokens[...] = jnp.where(wanted >= 0, logprob, 0.0)
    paid = [meta[samples : samples + 1, :].astype(F32) for meta in metas]
    reward_sum = functools.reduce(lambda a, b: a + b, [jnp.sum(row) for row in paid])
    lane = iota((1, slots), 1)
    objective = jnp.float32(0)
    for k in range(columns):
        for i in range(samples):
            at = k * samples + i
            score = jnp.sum(tokens[at : at + 1, :]) / length
            reward = jnp.sum(jnp.where(lane == i, paid[k], 0.0))
            advantage = reward - (reward_sum - reward) / (prompts - 1)
            objective += advantage * score

            @pl.when(where == k)
            def _(score=score, advantage=advantage, i=i):
                scores_out[i] = score
                advantages_out[i] = advantage

    objective_out[0] = -(objective / prompts)
    mine = tokens[:samples, :]
    for k in range(1, columns):
        mine = jnp.where(where == k, tokens[k * samples : (k + 1) * samples, :], mine)
    piece = mine[:, :cap]
    for n in range(1, slots // cap):
        piece = jnp.where(seq_at == n, mine[:, n * cap : (n + 1) * cap], piece)
    tokens_out[...] = piece


def close(stats, metas, relative, samples, cap, length):
    columns = lax.axis_size("sample")
    outs = (
        jax.ShapeDtypeStruct((samples, cap), F32),
        jax.ShapeDtypeStruct((samples,), F32),
        jax.ShapeDtypeStruct((samples,), F32),
        jax.ShapeDtypeStruct((1,), F32),
    )
    return call(
        functools.partial(close_kernel, relative, columns, length),
        outs,
        [stats, *metas],
        [vmem()] * (1 + len(metas)),
        out_specs=(vmem(), smem(), smem(), smem()),
        scratch=[pltpu.VMEM((stats.shape[1], stats.shape[2] // 2), F32)],
    )


def steps(
    queries, key_states, value_states, residual, out_weight, norm_gain,
    vocab_head, targets, scored_slots, lengths, rewards,
):
    samples, block, width = queries.shape
    model_width = out_weight.shape[1]
    seq_size, sample_size, vocab_size = (lax.axis_size(axis) for axis in CELL)
    cap = scored_slots.shape[1] // seq_size
    length = targets.shape[1]
    rows = samples * cap
    sizes = tuple(lax.axis_size(axis) for axis in ("groups",) + CELL)
    short = sizes == (2, 4, 2, 2) and samples == seq_size and key_states.shape[2] == HD

    def send(array, target):
        pairs = []
        for z in range(seq_size):
            for x in range(sample_size):
                for c in range(vocab_size):
                    place = target(z, x, c)
                    if place is not None:
                        source = (z * sample_size + x) * vocab_size + c
                        to = (place[0] * sample_size + place[1]) * vocab_size + place[2]
                        pairs.append((source, to))
        return lax.ppermute(array, CELL, pairs)

    def aside(array):
        pairs = []
        for g in range(2):
            for z in range(seq_size):
                for x in range(sample_size):
                    at = ((g * seq_size + z) * sample_size + x) * vocab_size
                    pairs.append((at, (((1 - g) * seq_size + z) * sample_size + x) * vocab_size))
                    pairs.append((at + 1, ((g * seq_size + z) * sample_size + 1 - x) * vocab_size + 1))
        return lax.ppermute(array, ("groups",) + CELL, pairs)

    def across(array):
        return send(array, lambda z, x, c: (z, x, c ^ 1))

    def beside(array):
        return send(array, lambda z, x, c: (z, x ^ 1, c))

    flips = (0, 2, 3, 1)
    if short:
        half_width = model_width // vocab_size
        parcel_rows = 2 * block + (width + half_width) // HD * cap
        parcels = call(
            functools.partial(parcel_kernel, flips),
            tuple(jax.ShapeDtypeStruct((parcel_rows, HD), BF16) for _ in flips),
            [keep(a) for a in (scored_slots, key_states, value_states, queries, residual)],
            [hbm()] * 5,
            scratch=[
                pltpu.VMEM(scored_slots.shape, jnp.int32),
                pltpu.VMEM(queries.shape, BF16),
                pltpu.VMEM((samples, block, half_width), BF16),
                pltpu.SemaphoreType.DMA((1 + 4 * len(flips),)),
            ],
        )
        far = send(parcels[1], lambda z, x, c: (z ^ 2, x, c))
        wrap = send(parcels[2], lambda z, x, c: (z ^ 3, x, c))
        near = send(parcels[3], lambda z, x, c: (z ^ 1, x, c))
        blocks = [parcels[0], far, wrap, near]
    else:
        offsets = (0,)
        kv_shape = (samples, block, 2 * key_states.shape[2])
        pair = call(
            pack_kernel,
            jax.ShapeDtypeStruct(kv_shape, BF16),
            [keep(key_states), keep(value_states)],
            [hbm(), hbm()],
            scratch=[pltpu.SemaphoreType.DMA((2,))],
            limit=4,
        )
        blocks = [lax.all_gather(pair, "seq", axis=1, tiled=True)]
    heads = width // HD
    slots, picked, picked_resid, meta, weight, gain = call(
        prep_kernel,
        (
            jax.ShapeDtypeStruct(scored_slots.shape, jnp.int32),
            jax.ShapeDtypeStruct((samples, heads * cap, HD), BF16),
            jax.ShapeDtypeStruct((rows, model_width), BF16),
            jax.ShapeDtypeStruct((samples + 1, scored_slots.shape[1]), jnp.int32),
            pltpu.VMEM(out_weight.shape, BF16),
            pltpu.VMEM((1, model_width), F32),
        ),
        [
            keep(array)
            for array in (
                scored_slots, targets, lengths, rewards, queries, residual,
                out_weight, norm_gain,
            )
        ],
        [hbm()] * 8,
        scratch=[
            pltpu.VMEM(targets.shape, jnp.int32),
            pltpu.SMEM(lengths.shape, jnp.int32),
            pltpu.SMEM(rewards.shape, jnp.int32),
            pltpu.VMEM(queries.shape, BF16),
            pltpu.VMEM(residual.shape, BF16),
            pltpu.SemaphoreType.DMA((8,)),
        ],
        limit=12,
    )
    head = pltpu.with_memory_space_constraint(vocab_head, pltpu.VMEM)
    weight = pltpu.with_memory_space_constraint(weight, pltpu.VMEM)
    if short:
        partial_value = call(
            functools.partial(completion_kernel, flips, block),
            jax.ShapeDtypeStruct((rows, model_width + half_width), BF16),
            [slots, weight, *blocks],
            [vmem()] * (2 + len(blocks)),
            scratch=[pltpu.VMEM((rows, width), BF16)],
            flops=10**10,
        )
    else:
        partial_value = call(
            functools.partial(attend_kernel, offsets),
            jax.ShapeDtypeStruct((rows, model_width), BF16),
            [slots, picked, weight, *blocks],
            [vmem()] * (3 + len(blocks)),
        )
    if short:
        other_meta = beside(meta)
        other_partial = across(partial_value)
        normed, half = call(
            pair_norm_kernel,
            (
                jax.ShapeDtypeStruct((rows, model_width), BF16),
                jax.ShapeDtypeStruct((rows // 2, model_width), BF16),
            ),
            [partial_value, other_partial, gain],
            [vmem()] * 3,
        )
        split = send(normed, lambda z, x, c: (z ^ (1, 3)[c], x, c))
        side = beside(half)
        turn = send(split, lambda z, x, c: (z, x ^ 1, c) if c == 0 else (z ^ 1, x, c))
        split_side = aside(split)
        side_far = send(side, lambda z, x, c: (z ^ 2, x, c))
        split_other = across(split)
        side_other = across(side)
        turn_other = across(turn)
        split_side_other = across(split_side)
        side_far_other = across(side_far)
        near = [(0, 0, 1), (0, (1, 3), 1), (0, (3, 1), 1), (1, 0, 2)]
        rest = [((1, 0), (1, 2), 1), ((0, 1), (2, 1), 1), (1, 3, -2), (1, 2, 2)]
        first = column_scores(
            head, meta, other_meta, near, [normed, split, split_other, side, side_other]
        )
        stats = column_scores(
            head, meta, other_meta, rest,
            [turn, turn_other, split_side, split_side_other, side_far, side_far_other],
            last=near, before=first,
        )
        stats = lax.all_to_all(stats, CELL, 0, 0, tiled=True)
        return close(stats, [meta, other_meta], True, samples, cap, length)
    summed = lax.psum(partial_value, "vocab")
    normed = call(
        lambda a, b, r, g, out: norm_kernel(a, b, r, g, out, None),
        jax.ShapeDtypeStruct((rows, model_width), BF16),
        [summed, jnp.zeros_like(summed), picked_resid, gain],
        [vmem()] * 4,
    )
    every = lax.all_gather(normed, "seq", axis=0, tiled=True)
    every = lax.all_gather(every, "sample", axis=0, tiled=True)
    metas = lax.all_gather(meta, "sample", axis=0)
    by_chip = (sample_size, samples, seq_size, cap)
    wanted = metas[:, :samples].reshape(by_chip).transpose(0, 2, 1, 3).reshape(1, -1)
    logs, picks = tiled_scores(vocab_head, every, wanted)
    top = lax.pmax(logs, CELL)
    total, pick = lax.psum((jnp.exp(logs - top), picks), CELL)
    by_row = (sample_size, seq_size, samples, cap)
    stats = [
        part.reshape(by_row).transpose(0, 2, 1, 3).reshape(1, sample_size * samples, seq_size * cap)
        for part in (top + jnp.log(total), pick)
    ]
    stats = jnp.concatenate(stats, axis=2)
    metas = [metas[k] for k in range(sample_size)]
    return close(stats, metas, False, samples, cap, length)


def solution(mesh):
    in_specs = (
        P(("groups", "sample"), "seq", "vocab"),
        P(("groups", "sample"), "seq", "vocab"),
        P(("groups", "sample"), "seq", "vocab"),
        P(("groups", "sample"), "seq", None),
        P("vocab", None),
        P(),
        P(("seq", "sample", "vocab"), None),
        P(("groups", "sample"), None),
        P(("groups", "sample"), None),
        P(("groups", "sample")),
        P(("groups", "sample")),
    )
    out_specs = (
        P(("groups", "sample"), "seq"),
        P(("groups", "sample")),
        P(("groups", "sample")),
        P("groups"),
    )
    step = jax.shard_map(steps, mesh=mesh, in_specs=in_specs, out_specs=out_specs, check_vma=False)
    if tuple(mesh.shape[axis] for axis in ("groups",) + CELL) != (2, 4, 2, 2):
        return step
    return step
```
